32 devices in a mesh: dp: 4 (over y, x), spatial: 8 (over z, core).
Axes of the slice: x: 2, y: 2, z: 4, core: 2. Of those that a mesh axis runs over, the one named last changes fastest.
Arguments:
- volume: bfloat16 [4, 16, 16, 8, 128], P('dp', 'spatial'), may hold values from -6 to 6
- cotangent: bfloat16 [4, 16, 16, 8, 128], P('dp', 'spatial'), may hold values from -6 to 6
- master: float32 [3456, 128], P('dp'), may hold values from -0.109375 to 0.109375
- moment: float32 [3456, 128], P('dp'), may hold values from -6 to 6
- second: float32 [3456, 128], P('dp'), may hold values from 0.25 to 4
Outputs:
- activation: bfloat16 [4, 16, 16, 8, 128], P('dp', 'spatial')
- input_grad: bfloat16 [4, 16, 16, 8, 128], P('dp', 'spatial')
- master_next: float32 [3456, 128], P('dp')
- moment_next: float32 [3456, 128], P('dp')
- second_next: float32 [3456, 128], P('dp')
The draws below stay inside these ranges and needn't reach their ends.
All inputs are finite; a program needn't handle non-finite values.
Results may differ from the reference program's by a relative error of at most 0.002.
The reference program's roundings to bfloat16 on the way (of `kernel` and `hidden_grad`) count: a program that leaves them out, or rounds other values in their place, can miss the bound.
Values may be sent and summed in bfloat16 or wider, within the bound.
A program may use at most 64 MiB of HBM per device.

```python
import math
import jax
import jax.numpy as jnp
from jax import lax

C = 128
TAPS = 27
NY = 16
NX = 8
NZ = 16
BATCH = 4


def spiked(drawn, rng, source, target, shards_of, factor):
    owner, partner = [(jnp.arange(drawn.shape[axis_at]) // (drawn.shape[axis_at] // shards_of)).reshape([-1 if axis == axis_at else 1 for axis in range(drawn.ndim)]) for axis_at in (source, target)]
    chosen = jax.random.permutation(rng, shards_of)[partner]
    strong = (owner == chosen) | (owner == (partner + shards_of // 2) % shards_of)
    return jnp.where(strong, factor * drawn, drawn)


def levels(rng, extent, shards, least, largest):
    level, own = 1.0, jax.random.fold_in(rng, 6)
    for dim, shards_of in shards:
        steps = jnp.exp(jax.random.uniform(jax.random.fold_in(own, dim), (shards_of,), jnp.float32, least / len(shards), largest / len(shards)))
        level = level * jnp.repeat(steps, extent[dim] // shards_of).reshape([-1 if axis == dim else 1 for axis in range(len(extent))])
    return level


def centred(own_key, dims, scale, bound, pieces=(), kind=jnp.bfloat16):
    loudness = levels(own_key, dims, pieces, -0.22, 0.18) if pieces else 1.0
    array = jax.random.normal(own_key, dims, jnp.float32) * scale * loudness
    return jnp.minimum(jnp.maximum(array, -bound), bound).astype(kind)


def heavy_noise(own_key, extent, scale, bound, cuts, heavy, kind=jnp.bfloat16):
    drawn = scale * jax.random.normal(own_key, extent, jnp.float32)
    if cuts:
        drawn = drawn * levels(own_key, extent, cuts, -0.22, 0.18)
    return jnp.clip(spiked(drawn, jax.random.fold_in(own_key, 3), *heavy), -bound, bound).astype(kind)


def setup_inputs(seed: int = 0) -> dict:
    seeds = jax.random.split(jax.random.key(seed), 6)
    volume = heavy_noise(seeds[0], (BATCH, NZ, NY, NX, C), 1.0, 6.0, ((0, 4), (1, 8)), (1, 4, 8, 2.0))
    cotangent = centred(seeds[1], (BATCH, NZ, NY, NX, C), 1.0, 6.0, ((0, 4), (1, 8)))
    master = centred(seeds[2], (TAPS * C, C), (TAPS * C) ** -0.5, 0.109375, ((0, 4),), jnp.float32)
    moment = centred(seeds[3], (TAPS * C, C), 1.0, 6.0, ((0, 4),), jnp.float32)
    second = jnp.clip(jnp.exp(math.log(4.0) - 2.7725887 * jax.random.uniform(seeds[4], (TAPS * C, C), jnp.float32) ** levels(seeds[4], (TAPS * C, C), ((0, 4),), -0.2, 0.2)), 0.25, 4.0)
    return {"volume": volume, "cotangent": cotangent, "master": master, "moment": moment, "second": second}


def convolve(inputs, weights):
    return lax.conv_general_dilated(inputs, weights, (1, 1, 1), 'SAME', dimension_numbers=('NDHWC', 'DHWIO', 'NDHWC'), precision=lax.Precision.HIGHEST)

def reference(volume, cotangent, master, moment, second):
    width = master.shape[1]
    rounded = lax.optimization_barrier(master.astype(jnp.bfloat16))
    kernel = rounded.astype(jnp.float32).reshape(3, 3, 3, width, width)
    field = volume.astype(jnp.float32)
    preact, pullback = jax.vjp(convolve, field, kernel)
    activation = jax.nn.silu(preact).astype(jnp.bfloat16)
    sigma = jax.nn.sigmoid(preact)
    slope = sigma * (1.0 + preact * (1.0 - sigma))
    hidden_grad = lax.optimization_barrier((cotangent.astype(jnp.float32) * slope).astype(jnp.bfloat16))
    input_full, weight_full = pullback(hidden_grad.astype(jnp.float32))
    input_grad = input_full.astype(jnp.bfloat16)
    weight_grad = weight_full.reshape(27 * width, width) / math.sqrt(BATCH * NZ * NY * NX)
    moment_next = 0.9 * moment + 0.1 * weight_grad
    second_next = 0.999 * second + 0.001 * weight_grad * weight_grad
    master_next = master - 0.001 * (moment_next / (jnp.sqrt(second_next) + 1e-08) + 0.01 * master)
    return (activation, input_grad, master_next, moment_next, second_next)
```

```python
import functools
import math

import jax
import jax.numpy as jnp
from jax import lax
from jax.experimental import pallas as pl
from jax.experimental.pallas import tpu as pltpu
from jax.sharding import PartitionSpec as P

MESH = pl.DeviceIdType.MESH
TILE = 16
CORES = 2


def shifted(plane, cols, step_y, step_x):
    area, width = plane.shape
    column = lax.broadcasted_iota(jnp.int32, (area, width), 0) % cols
    if step_x < 0:
        plane = jnp.where(column == 0, 0.0, pltpu.roll(plane, 1, 0))
    elif step_x > 0:
        plane = jnp.where(column == cols - 1, 0.0, pltpu.roll(plane, area - 1, 0))
    edge = jnp.zeros((cols, width), jnp.float32)
    if step_y < 0:
        plane = jnp.concatenate([edge, plane[: area - cols]], axis=0)
    elif step_y > 0:
        plane = jnp.concatenate([plane[cols:], edge], axis=0)
    return plane


def layer_kernel(
    sizes,
    volume,
    cotangent,
    master,
    moment,
    second,
    activation,
    input_grad,
    master_next,
    moment_next,
    second_next,
    kernel,
    halo,
    grad_halo,
    hidden,
    columns,
    turned,
    local_grad,
    local_sent,
    pair_got,
    chip_sent,
    chip_got,
    own_sum,
    slab_sent,
    slab_got,
    total,
    halo_s,
    halo_r,
    gh_s,
    gh_r,
    ag_s,
    ag_r,
    fw_s,
    fw_r,
    pr_s,
    pr_r,
    ch_s,
    ch_r,
    sl_s,
    sl_r,
    to_s,
    to_r,
    tf_s,
    tf_r,
):
    dps, slabs, planes, area, cols, cells_all = sizes
    chips = slabs // CORES
    width = volume.shape[1]
    rows = master.shape[0]
    half = rows // CORES
    piece = total.shape[2]
    dp = lax.axis_index("dp")
    slab = lax.axis_index("spatial")
    core = slab % CORES
    chip = slab // CORES
    other = 1 - core
    pair = chip * CORES + other
    block = planes * area

    def copy(src, dst, send, recv, target):
        return pltpu.make_async_remote_copy(
            src_ref=src,
            dst_ref=dst,
            send_sem=send,
            recv_sem=recv,
            device_id=target,
            device_id_type=MESH,
        )

    barrier = pltpu.get_barrier_semaphore()
    for step in range(1, dps):
        pl.semaphore_signal(
            barrier, inc=1, device_id=((dp + step) % dps, slab), device_id_type=MESH
        )
    for step in range(1, slabs):
        pl.semaphore_signal(
            barrier, inc=1, device_id=(dp, (slab + step) % slabs), device_id_type=MESH
        )

    def kernel_half(shard, which):
        return kernel.at[pl.ds(pl.multiple_of(shard * rows + which * half, TILE), half)]

    kernel[pl.ds(pl.multiple_of(dp * rows, TILE), rows)] = master[...].astype(jnp.bfloat16)
    pl.semaphore_wait(barrier, dps - 1 + slabs - 1)

    def halo_copy(source, dest, send, recv, side):
        if side == 0:
            return copy(
                source.at[pl.ds(block - area, area)], dest.at[0], send.at[0], recv.at[0], (dp, slab + 1)
            )
        return copy(source.at[pl.ds(0, area)], dest.at[1], send.at[1], recv.at[1], (dp, slab - 1))

    def halo_start(source, dest, send, recv):
        @pl.when(slab < slabs - 1)
        def _():
            halo_copy(source, dest, send, recv, 0).start()

        @pl.when(slab > 0)
        def _():
            halo_copy(source, dest, send, recv, 1).start()

    def halo_sent(source, dest, send, recv):
        @pl.when(slab < slabs - 1)
        def _():
            halo_copy(source, dest, send, recv, 0).wait_send()

        @pl.when(slab > 0)
        def _():
            halo_copy(source, dest, send, recv, 1).wait_send()

    def halo_wait(source, dest, send, recv):
        @pl.when(slab > 0)
        def _():
            halo_copy(source, dest, send, recv, 0).wait_recv()

        @pl.when(slab < slabs - 1)
        def _():
            halo_copy(source, dest, send, recv, 1).wait_recv()

        @pl.when(slab == 0)
        def _():
            dest[0] = jnp.zeros((area, width), jnp.bfloat16)

        @pl.when(slab == slabs - 1)
        def _():
            dest[1] = jnp.zeros((area, width), jnp.bfloat16)

    def gather_copy(shard, target):
        mine = kernel_half(shard, core)
        return copy(mine, mine, ag_s.at[target], ag_r.at[shard], (target, slab))

    def relay_copy(shard, which):
        mine = kernel_half(shard, which)
        return copy(mine, mine, fw_s.at[shard], fw_r.at[shard], (dp, pair))

    for step in range(1, dps):
        gather_copy(dp, (dp + step) % dps).start()
    halo_start(volume, halo, halo_s, halo_r)

    def put_columns(plane, at, sign, turn):
        plane = plane.astype(jnp.float32)
        for e in range(3):
            for f in range(3):
                moved = shifted(plane, cols, sign * (e - 1), sign * (f - 1)).astype(jnp.bfloat16)
                tap = e * 3 + f
                columns[at * area : (at + 1) * area, tap * width : (tap + 1) * width] = moved
                if turn:
                    turned[tap * width : (tap + 1) * width, at * area : (at + 1) * area] = moved.T

    for plane in range(planes):
        put_columns(volume[plane * area : (plane + 1) * area], plane + 1, 1, True)
    halo_wait(volume, halo, halo_s, halo_r)
    put_columns(halo[0], 0, 1, True)
    put_columns(halo[1], planes + 1, 1, True)

    for step in range(1, dps):
        source = (dp + step) % dps
        gather_copy(source, dp).wait_recv()
        relay_copy(source, core).start()
    for step in range(1, dps):
        relay_copy((dp + step) % dps, other).wait_recv()

    group = 9 * width
    preact = jnp.zeros((block, width), jnp.float32)
    for a in range(3):
        preact = preact + jnp.dot(
            columns[a * area : a * area + block, :],
            kernel[a * group : (a + 1) * group, :],
            preferred_element_type=jnp.float32,
        )
    sigma = jax.nn.sigmoid(preact)
    activation[...] = (preact * sigma).astype(jnp.bfloat16)
    slope = sigma * (1.0 + preact * (1.0 - sigma))
    hidden[...] = (cotangent[...].astype(jnp.float32) * slope).astype(jnp.bfloat16)

    def pair_copy(shard, which):
        at = pl.ds(pl.multiple_of(shard * rows + which * half, TILE), half)
        return copy(
            local_sent.at[at], pair_got.at[shard], pr_s.at[shard], pr_r.at[shard], (dp, pair)
        )

    next_shard = 0
    for a in range(3):
        part = jnp.dot(
            turned[:, a * area : a * area + block],
            hidden[...],
            preferred_element_type=jnp.float32,
        )
        local_grad[a * group : (a + 1) * group, :] = part
        local_sent[a * group : (a + 1) * group, :] = part.astype(jnp.bfloat16)
        while next_shard < dps and (next_shard + 1) * rows <= (a + 1) * group:
            pair_copy(next_shard, other).start()
            next_shard += 1
        if a == 0:
            halo_start(hidden, grad_halo, gh_s, gh_r)

    def own_rows(shard):
        return local_grad[pl.ds(pl.multiple_of(shard * rows + core * half, TILE), half), :]

    def chip_copy(shard, source):
        return copy(
            chip_sent.at[shard], chip_got.at[source], ch_s.at[shard], ch_r.at[source], (shard, slab)
        )

    for step in range(1, dps):
        shard = (dp + step) % dps
        pair_copy(shard, core).wait_recv()
        chip_sent[shard] = (own_rows(shard) + pair_got[shard].astype(jnp.float32)).astype(
            jnp.bfloat16
        )
        chip_copy(shard, dp).start()
    pair_copy(dp, core).wait_recv()
    own_sum[...] = own_rows(dp) + pair_got[dp].astype(jnp.float32)

    halo_wait(hidden, grad_halo, gh_s, gh_r)
    for plane in range(planes):
        put_columns(hidden[plane * area : (plane + 1) * area], plane + 1, -1, False)
    put_columns(grad_halo[0], 0, -1, False)
    put_columns(grad_halo[1], planes + 1, -1, False)
    back = jnp.zeros((block, width), jnp.float32)
    for a in range(3):
        for tap in range(9):
            at = (a * 9 + tap) * width
            back = back + lax.dot_general(
                columns[(2 - a) * area : (2 - a) * area + block, tap * width : (tap + 1) * width],
                kernel[at : at + width, :],
                (((1,), (1,)), ((), ())),
                preferred_element_type=jnp.float32,
            )
    input_grad[...] = back.astype(jnp.bfloat16)

    for step in range(1, dps):
        source = (dp + step) % dps
        chip_copy(dp, source).wait_recv()
        own_sum[...] += chip_got[source].astype(jnp.float32)
    slab_sent[...] = own_sum[...].astype(jnp.bfloat16)

    def start_of(index):
        return jnp.minimum(index * piece, half - piece)

    def slab_copy(owner, source):
        at = pl.ds(pl.multiple_of(start_of(owner), TILE), piece)
        return copy(
            slab_sent.at[at],
            slab_got.at[source],
            sl_s.at[owner],
            sl_r.at[source],
            (dp, owner * CORES + core),
        )

    for step in range(1, chips):
        slab_copy((chip + step) % chips, chip).start()
    piece_sum = own_sum[pl.ds(pl.multiple_of(start_of(chip), TILE), piece), :]
    for step in range(1, chips):
        source = (chip + step) % chips
        slab_copy(chip, source).wait_recv()
        piece_sum = piece_sum + slab_got[source].astype(jnp.float32)
    total[core, chip] = piece_sum.astype(jnp.bfloat16)

    def total_copy(source, target):
        ref = total.at[core, source]
        return copy(ref, ref, to_s.at[target], to_r.at[source], (dp, target * CORES + core))

    def total_relay(source, which):
        ref = total.at[which, source]
        return copy(ref, ref, tf_s.at[source], tf_r.at[source], (dp, pair))

    for step in range(1, chips):
        total_copy(chip, (chip + step) % chips).start()
    total_relay(chip, core).start()
    for step in range(1, chips):
        source = (chip + step) % chips
        total_copy(source, chip).wait_recv()
        total_relay(source, core).start()
    for step in range(chips):
        total_relay((chip + step) % chips, other).wait_recv()

    scale = 1.0 / math.sqrt(cells_all)
    for which in range(CORES):
        for index in range(chips):
            at = which * half + min(index * piece, half - piece)
            end = at + piece
            grad = total[which, index].astype(jnp.float32) * scale
            old = master[at:end, :]
            first = 0.9 * moment[at:end, :] + 0.1 * grad
            square = 0.999 * second[at:end, :] + 0.001 * grad * grad
            moment_next[at:end, :] = first
            second_next[at:end, :] = square
            master_next[at:end, :] = old - 0.001 * (
                first / (jnp.sqrt(square) + 1e-08) + 0.01 * old
            )

    halo_sent(volume, halo, halo_s, halo_r)
    halo_sent(hidden, grad_halo, gh_s, gh_r)
    for step in range(1, dps):
        peer = (dp + step) % dps
        gather_copy(dp, peer).wait_send()
        relay_copy(peer, core).wait_send()
        chip_copy(peer, dp).wait_send()
    for shard in range(dps):
        pair_copy(shard, other).wait_send()
    for step in range(1, chips):
        peer = (chip + step) % chips
        slab_copy(peer, chip).wait_send()
        total_copy(chip, peer).wait_send()
    for index in range(chips):
        total_relay(index, core).wait_send()


def per_device(volume, cotangent, master, moment, second):
    _, planes, lines, cols, width = volume.shape
    rows = master.shape[0]
    dps = lax.axis_size("dp")
    slabs = lax.axis_size("spatial")
    chips = slabs // CORES
    area = lines * cols
    block = planes * area
    half = rows // CORES
    piece = min(half, -(-half // (chips * TILE)) * TILE)
    cells_all = dps * slabs * block
    bf16, f32 = jnp.bfloat16, jnp.float32
    dma = pltpu.SemaphoreType.DMA
    vmem = pl.BlockSpec(memory_space=pltpu.VMEM)
    sizes = (dps, slabs, planes, area, cols, cells_all)
    activation, input_grad, master_next, moment_next, second_next = pl.pallas_call(
        functools.partial(layer_kernel, sizes),
        name="layer",
        out_shape=[
            jax.ShapeDtypeStruct((block, width), bf16),
            jax.ShapeDtypeStruct((block, width), bf16),
            jax.ShapeDtypeStruct((rows, width), f32),
            jax.ShapeDtypeStruct((rows, width), f32),
            jax.ShapeDtypeStruct((rows, width), f32),
        ],
        in_specs=[vmem] * 5,
        out_specs=[vmem] * 5,
        scratch_shapes=[
            pltpu.VMEM((dps * rows, width), bf16),
            pltpu.VMEM((2, area, width), bf16),
            pltpu.VMEM((2, area, width), bf16),
            pltpu.VMEM((block, width), bf16),
            pltpu.VMEM((block + 2 * area, 9 * width), bf16),
            pltpu.VMEM((9 * width, block + 2 * area), bf16),
            pltpu.VMEM((dps * rows, width), f32),
            pltpu.VMEM((dps * rows, width), bf16),
            pltpu.VMEM((dps, half, width), bf16),
            pltpu.VMEM((dps, half, width), bf16),
            pltpu.VMEM((dps, half, width), bf16),
            pltpu.VMEM((half, width), f32),
            pltpu.VMEM((half, width), bf16),
            pltpu.VMEM((chips, piece, width), bf16),
            pltpu.VMEM((CORES, chips, piece, width), bf16),
            dma((2,)),
            dma((2,)),
            dma((2,)),
            dma((2,)),
            dma((dps,)),
            dma((dps,)),
            dma((dps,)),
            dma((dps,)),
            dma((dps,)),
            dma((dps,)),
            dma((dps,)),
            dma((dps,)),
            dma((chips,)),
            dma((chips,)),
            dma((chips,)),
            dma((chips,)),
            dma((chips,)),
            dma((chips,)),
        ],
        compiler_params=pltpu.CompilerParams(
            collective_id=0, has_side_effects=True, vmem_limit_bytes=48 * 1024 * 1024
        ),
    )(
        volume.reshape(block, width),
        cotangent.reshape(block, width),
        master,
        moment,
        second,
    )
    return (
        activation.reshape(volume.shape),
        input_grad.reshape(volume.shape),
        master_next,
        moment_next,
        second_next,
    )


def solution(mesh):
    field = P("dp", "spatial", None, None, None)
    shard = P("dp", None)
    return jax.shard_map(
        per_device,
        mesh=mesh,
        in_specs=(field, field, shard, shard, shard),
        out_specs=(field, field, shard, shard, shard),
        check_vma=False,
    )
```

```python
import functools
import math

import jax
import jax.numpy as jnp
from jax import lax
from jax.experimental import pallas as pl
from jax.experimental.pallas import tpu as pltpu
from jax.sharding import PartitionSpec as P

MESH = pl.DeviceIdType.MESH
TILE = 16
PARTS = 3
VMEM_BYTES = 67043328
SLACK = 48 * 1024
CORES = 2


def shifted(plane, cols, step_y, step_x):
    area, width = plane.shape
    column = lax.broadcasted_iota(jnp.int32, (area, width), 0) % cols
    if step_x < 0:
        plane = jnp.where(column == 0, 0.0, pltpu.roll(plane, 1, 0))
    elif step_x > 0:
        plane = jnp.where(column == cols - 1, 0.0, pltpu.roll(plane, area - 1, 0))
    edge = jnp.zeros((cols, width), jnp.float32)
    if step_y < 0:
        plane = jnp.concatenate([edge, plane[: area - cols]], axis=0)
    elif step_y > 0:
        plane = jnp.concatenate([plane[cols:], edge], axis=0)
    return plane


def layer_kernel(
    sizes,
    volume_hbm,
    cotangent_hbm,
    master_hbm,
    moment_hbm,
    second_hbm,
    activation,
    input_grad,
    master_next,
    moment_next,
    second_next,
    volume,
    cotangent,
    master,
    moment,
    second,
    kernel,
    halo,
    grad_halo,
    hidden,
    columns,
    turned,
    local_grad,
    local_sent,
    pair_got,
    chip_sent,
    chip_got,
    own_sum,
    chain_sent,
    chain_got,
    total,
    load_s,
    halo_s,
    halo_r,
    gh_s,
    gh_r,
    ag_s,
    ag_r,
    fw_s,
    fw_r,
    pr_s,
    pr_r,
    ch_s,
    ch_r,
    sl_s,
    sl_r,
    to_s,
    to_r,
    tf_s,
    tf_r,
):
    dps, slabs, planes, area, cols, cells_all = sizes
    chips = slabs // CORES
    width = volume.shape[1]
    rows = master.shape[0]
    half = rows // CORES
    part_rows = half // PARTS
    dp = lax.axis_index("dp")
    slab = lax.axis_index("spatial")
    core = slab % CORES
    chip = slab // CORES
    other = 1 - core
    pair = chip * CORES + other
    block = planes * area

    def copy(src, dst, send, recv, target):
        return pltpu.make_async_remote_copy(
            src_ref=src,
            dst_ref=dst,
            send_sem=send,
            recv_sem=recv,
            device_id=target,
            device_id_type=MESH,
        )

    loads = [
        pltpu.make_async_copy(source, dest, load_s.at[index])
        for index, (source, dest) in enumerate(
            (
                (master_hbm, master),
                (volume_hbm, volume),
                (cotangent_hbm, cotangent),
                (moment_hbm, moment),
                (second_hbm, second),
            )
        )
    ]
    for load in loads:
        load.start()

    barrier = pltpu.get_barrier_semaphore()
    for step in range(1, dps):
        pl.semaphore_signal(
            barrier, inc=1, device_id=((dp + step) % dps, slab), device_id_type=MESH
        )
    for step in range(1, slabs):
        pl.semaphore_signal(
            barrier, inc=1, device_id=(dp, (slab + step) % slabs), device_id_type=MESH
        )

    def kernel_half(shard, which):
        return kernel.at[pl.ds(pl.multiple_of(shard * rows + which * half, TILE), half)]

    loads[0].wait()
    kernel[pl.ds(pl.multiple_of(dp * rows, TILE), rows)] = master[...].astype(jnp.bfloat16)
    pl.semaphore_wait(barrier, dps - 1 + slabs - 1)

    def halo_copy(source, dest, send, recv, side):
        if side == 0:
            return copy(
                source.at[pl.ds(block - area, area)], dest.at[0], send.at[0], recv.at[0], (dp, slab + 1)
            )
        return copy(source.at[pl.ds(0, area)], dest.at[1], send.at[1], recv.at[1], (dp, slab - 1))

    def halo_start(source, dest, send, recv):
        @pl.when(slab < slabs - 1)
        def _():
            halo_copy(source, dest, send, recv, 0).start()

        @pl.when(slab > 0)
        def _():
            halo_copy(source, dest, send, recv, 1).start()

    def halo_sent(source, dest, send, recv):
        @pl.when(slab < slabs - 1)
        def _():
            halo_copy(source, dest, send, recv, 0).wait_send()

        @pl.when(slab > 0)
        def _():
            halo_copy(source, dest, send, recv, 1).wait_send()

    def halo_wait(source, dest, send, recv):
        @pl.when(slab > 0)
        def _():
            halo_copy(source, dest, send, recv, 0).wait_recv()

        @pl.when(slab < slabs - 1)
        def _():
            halo_copy(source, dest, send, recv, 1).wait_recv()

        @pl.when(slab == 0)
        def _():
            dest[0] = jnp.zeros((area, width), jnp.bfloat16)

        @pl.when(slab == slabs - 1)
        def _():
            dest[1] = jnp.zeros((area, width), jnp.bfloat16)

    def gather_copy(shard, target):
        mine = kernel_half(shard, core)
        return copy(mine, mine, ag_s.at[target], ag_r.at[shard], (target, slab))

    def relay_copy(shard, which):
        mine = kernel_half(shard, which)
        return copy(mine, mine, fw_s.at[shard], fw_r.at[shard], (dp, pair))

    for step in range(1, dps):
        gather_copy(dp, (dp + step) % dps).start()
    loads[1].wait()
    halo_start(volume, halo, halo_s, halo_r)

    def put_columns(plane, at, sign, turn):
        plane = plane.astype(jnp.float32)
        for e in range(3):
            for f in range(3):
                moved = shifted(plane, cols, sign * (e - 1), sign * (f - 1)).astype(jnp.bfloat16)
                tap = e * 3 + f
                columns[at * area : (at + 1) * area, tap * width : (tap + 1) * width] = moved
                if turn:
                    turned[tap * width : (tap + 1) * width, at * area : (at + 1) * area] = moved.T

    for plane in range(planes):
        put_columns(volume[plane * area : (plane + 1) * area], plane + 1, 1, True)
    halo_wait(volume, halo, halo_s, halo_r)
    put_columns(halo[0], 0, 1, True)
    put_columns(halo[1], planes + 1, 1, True)

    for step in range(1, dps):
        source = (dp + step) % dps
        gather_copy(source, dp).wait_recv()
        relay_copy(source, core).start()
    for step in range(1, dps):
        relay_copy((dp + step) % dps, other).wait_recv()

    group = 9 * width
    preact = jnp.zeros((block, width), jnp.float32)
    for a in range(3):
        preact = preact + jnp.dot(
            columns[a * area : a * area + block, :],
            kernel[a * group : (a + 1) * group, :],
            preferred_element_type=jnp.float32,
        )
    loads[2].wait()
    sigma = jax.nn.sigmoid(preact)
    activation[...] = (preact * sigma).astype(jnp.bfloat16)
    slope = sigma * (1.0 + preact * (1.0 - sigma))
    hidden[...] = (cotangent[...].astype(jnp.float32) * slope).astype(jnp.bfloat16)

    def rows_of(k):
        return pl.ds(k * part_rows, part_rows)

    def pair_copy(shard, k, which):
        at = pl.ds(pl.multiple_of(shard * rows + which * half + k * part_rows, TILE), part_rows)
        flag = shard * PARTS + k
        return copy(
            local_sent.at[at], pair_got.at[shard, rows_of(k)], pr_s.at[flag], pr_r.at[flag], (dp, pair)
        )

    for a in range(3):
        part = jnp.dot(
            turned[:, a * area : a * area + block],
            hidden[...],
            preferred_element_type=jnp.float32,
        )
        local_grad[a * group : (a + 1) * group, :] = part
        local_sent[a * group : (a + 1) * group, :] = part.astype(jnp.bfloat16)
        if a == 0:
            halo_start(hidden, grad_halo, gh_s, gh_r)

    for k in range(PARTS):
        for step in range(dps):
            pair_copy((dp + step) % dps, k, other).start()

    def chip_rows(shard, k):
        pair_copy(shard, k, core).wait_recv()
        at = pl.multiple_of(shard * rows + core * half + k * part_rows, TILE)
        return local_grad[pl.ds(at, part_rows), :] + pair_got[shard, rows_of(k)].astype(jnp.float32)

    def chip_copy(shard, source, k):
        return copy(
            chip_sent.at[shard, rows_of(k)],
            chip_got.at[source, rows_of(k)],
            ch_s.at[shard * PARTS + k],
            ch_r.at[source * PARTS + k],
            (shard, slab),
        )

    for k in range(PARTS):
        for step in range(1, dps):
            shard = (dp + step) % dps
            chip_sent[shard, rows_of(k)] = chip_rows(shard, k).astype(jnp.bfloat16)
            chip_copy(shard, dp, k).start()
        own_sum[rows_of(k)] = chip_rows(dp, k)

    halo_wait(hidden, grad_halo, gh_s, gh_r)
    for plane in range(planes):
        put_columns(hidden[plane * area : (plane + 1) * area], plane + 1, -1, False)
    put_columns(grad_halo[0], 0, -1, False)
    put_columns(grad_halo[1], planes + 1, -1, False)
    back = jnp.zeros((block, width), jnp.float32)
    for a in range(3):
        for tap in range(9):
            at = (a * 9 + tap) * width
            back = back + lax.dot_general(
                columns[(2 - a) * area : (2 - a) * area + block, tap * width : (tap + 1) * width],
                kernel[at : at + width, :],
                (((1,), (1,)), ((), ())),
                preferred_element_type=jnp.float32,
            )
    input_grad[...] = back.astype(jnp.bfloat16)

    low = chip < chips // 2
    inner = jnp.where(low, chip + 1, chip - 1)
    outer = jnp.where(low, chip - 1, chip + 1)
    is_end = (chip == 0) | (chip == chips - 1)
    is_middle = (chip == chips // 2 - 1) | (chip == chips // 2)
    slot = jnp.where(is_middle, 1, 0)

    def chain_copy(at, k):
        flag = at * PARTS + k
        return copy(
            chain_sent.at[rows_of(k)],
            chain_got.at[at, rows_of(k)],
            sl_s.at[k],
            sl_r.at[flag],
            (dp, inner * CORES + core),
        )

    def total_copy(k):
        ref = total.at[core, rows_of(k)]
        return copy(ref, ref, to_s.at[k], to_r.at[k], (dp, outer * CORES + core))

    def total_relay(k, which):
        ref = total.at[which, rows_of(k)]
        return copy(ref, ref, tf_s.at[k], tf_r.at[k], (dp, pair))

    def reduce_rows(k):
        for step in range(1, dps):
            source = (dp + step) % dps
            chip_copy(dp, source, k).wait_recv()
            own_sum[rows_of(k)] += chip_got[source, rows_of(k)].astype(jnp.float32)

        @pl.when(is_end)
        def _():
            chain_sent[rows_of(k)] = own_sum[rows_of(k)].astype(jnp.bfloat16)
            chain_copy(slot, k).start()

    def pass_inward(k):
        @pl.when(jnp.logical_not(is_end))
        def _():
            chain_copy(0, k).wait_recv()
            chain_sent[rows_of(k)] = (
                own_sum[rows_of(k)] + chain_got[0, rows_of(k)].astype(jnp.float32)
            ).astype(jnp.bfloat16)
            chain_copy(slot, k).start()

    scale = 1.0 / math.sqrt(cells_all)

    def update(k, which):
        at = pl.ds(pl.multiple_of(which * half + k * part_rows, TILE), part_rows)
        grad = total[which, rows_of(k)].astype(jnp.float32) * scale
        old = master[at, :]
        first = 0.9 * moment[at, :] + 0.1 * grad
        square = 0.999 * second[at, :] + 0.001 * grad * grad
        moment_next[at, :] = first
        second_next[at, :] = square
        master_next[at, :] = old - 0.001 * (first / (jnp.sqrt(square) + 1e-08) + 0.01 * old)

    def finish(k):
        @pl.when(is_middle)
        def _():
            chain_copy(1, k).wait_recv()
            total[core, rows_of(k)] = (
                chain_sent[rows_of(k)].astype(jnp.float32)
                + chain_got[1, rows_of(k)].astype(jnp.float32)
            ).astype(jnp.bfloat16)

        @pl.when(jnp.logical_not(is_middle))
        def _():
            total_copy(k).wait_recv()

        @pl.when(jnp.logical_not(is_end))
        def _():
            total_copy(k).start()

        total_relay(k, core).start()
        if k == 0:
            loads[3].wait()
            loads[4].wait()
        update(k, core)

    for k in range(PARTS):
        reduce_rows(k)
        if k >= 1:
            pass_inward(k - 1)
    finish(0)
    pass_inward(PARTS - 1)
    for k in range(PARTS):
        if k >= 1:
            finish(k)
            total_relay(k - 1, other).wait_recv()
            update(k - 1, other)
    total_relay(PARTS - 1, other).wait_recv()
    update(PARTS - 1, other)

    halo_sent(volume, halo, halo_s, halo_r)
    halo_sent(hidden, grad_halo, gh_s, gh_r)
    for step in range(1, dps):
        peer = (dp + step) % dps
        gather_copy(dp, peer).wait_send()
        relay_copy(peer, core).wait_send()
        for k in range(PARTS):
            chip_copy(peer, dp, k).wait_send()
    for k in range(PARTS):
        for shard in range(dps):
            pair_copy(shard, k, other).wait_send()
        chain_copy(slot, k).wait_send()
        total_relay(k, core).wait_send()

        @pl.when(jnp.logical_not(is_end))
        def _():
            total_copy(k).wait_send()


def store_kernel(*refs):
    count = (len(refs) - 1) // 2
    flags = refs[-1]
    stores = [
        pltpu.make_async_copy(refs[index], refs[count + index], flags.at[index])
        for index in range(count)
    ]
    for store in stores:
        store.start()
    for store in stores:
        store.wait()


def per_device(volume, cotangent, master, moment, second):
    _, planes, lines, cols, width = volume.shape
    rows = master.shape[0]
    dps = lax.axis_size("dp")
    slabs = lax.axis_size("spatial")
    chips = slabs // CORES
    area = lines * cols
    block = planes * area
    half = rows // CORES
    cells_all = dps * slabs * block
    bf16, f32 = jnp.bfloat16, jnp.float32
    dma = pltpu.SemaphoreType.DMA
    vmem = pl.BlockSpec(memory_space=pltpu.VMEM)
    sizes = (dps, slabs, planes, area, cols, cells_all)
    out_shape = [
        jax.ShapeDtypeStruct((block, width), bf16),
        jax.ShapeDtypeStruct((block, width), bf16),
        jax.ShapeDtypeStruct((rows, width), f32),
        jax.ShapeDtypeStruct((rows, width), f32),
        jax.ShapeDtypeStruct((rows, width), f32),
    ]
    held = 2 * block * width * 2 + 3 * rows * width * 4
    grant = VMEM_BYTES - held - SLACK
    hbm = pl.BlockSpec(memory_space=pltpu.HBM)
    results = pl.pallas_call(
        functools.partial(layer_kernel, sizes),
        name="layer",
        out_shape=out_shape,
        in_specs=[hbm] * 5,
        out_specs=[vmem] * 5,
        scratch_shapes=[
            pltpu.VMEM((block, width), bf16),
            pltpu.VMEM((block, width), bf16),
            pltpu.VMEM((rows, width), f32),
            pltpu.VMEM((rows, width), f32),
            pltpu.VMEM((rows, width), f32),
            pltpu.VMEM((dps * rows, width), bf16),
            pltpu.VMEM((2, area, width), bf16),
            pltpu.VMEM((2, area, width), bf16),
            pltpu.VMEM((block, width), bf16),
            pltpu.VMEM((block + 2 * area, 9 * width), bf16),
            pltpu.VMEM((9 * width, block + 2 * area), bf16),
            pltpu.VMEM((dps * rows, width), f32),
            pltpu.VMEM((dps * rows, width), bf16),
            pltpu.VMEM((dps, half, width), bf16),
            pltpu.VMEM((dps, half, width), bf16),
            pltpu.VMEM((dps, half, width), bf16),
            pltpu.VMEM((half, width), f32),
            pltpu.VMEM((half, width), bf16),
            pltpu.VMEM((2, half, width), bf16),
            pltpu.VMEM((CORES, half, width), bf16),
            dma((5,)),
            dma((2,)),
            dma((2,)),
            dma((2,)),
            dma((2,)),
            dma((dps,)),
            dma((dps,)),
            dma((dps,)),
            dma((dps,)),
            dma((dps * PARTS,)),
            dma((dps * PARTS,)),
            dma((dps * PARTS,)),
            dma((dps * PARTS,)),
            dma((PARTS,)),
            dma((2 * PARTS,)),
            dma((PARTS,)),
            dma((PARTS,)),
            dma((PARTS,)),
            dma((PARTS,)),
        ],
        compiler_params=pltpu.CompilerParams(
            collective_id=0, has_side_effects=True, vmem_limit_bytes=grant
        ),
    )(
        volume.reshape(block, width),
        cotangent.reshape(block, width),
        master,
        moment,
        second,
    )
    activation, input_grad, master_next, moment_next, second_next = pl.pallas_call(
        store_kernel,
        name="store",
        out_shape=out_shape,
        in_specs=[vmem] * 5,
        out_specs=[hbm] * 5,
        scratch_shapes=[dma((5,))],
        compiler_params=pltpu.CompilerParams(vmem_limit_bytes=grant),
    )(*results)
    return (
        activation.reshape(volume.shape),
        input_grad.reshape(volume.shape),
        master_next,
        moment_next,
        second_next,
    )


def solution(mesh):
    field = P("dp", "spatial", None, None, None)
    shard = P("dp", None)
    return jax.shard_map(
        per_device,
        mesh=mesh,
        in_specs=(field, field, shard, shard, shard),
        out_specs=(field, field, shard, shard, shard),
        check_vma=False,
    )
```

```python
import functools
import math

import jax
import jax.numpy as jnp
from jax import lax
from jax.experimental import pallas as pl
from jax.experimental.pallas import tpu as pltpu
from jax.sharding import PartitionSpec as P

MESH = pl.DeviceIdType.MESH
TILE = 16
PARTS = 3
VMEM_BYTES = 67043328
SLACK = 48 * 1024
CORES = 2


def shifted(plane, cols, step_y, step_x):
    area, width = plane.shape
    column = lax.broadcasted_iota(jnp.int32, (area, width), 0) % cols
    if step_x < 0:
        plane = jnp.where(column == 0, 0.0, pltpu.roll(plane, 1, 0))
    elif step_x > 0:
        plane = jnp.where(column == cols - 1, 0.0, pltpu.roll(plane, area - 1, 0))
    edge = jnp.zeros((cols, width), jnp.float32)
    if step_y < 0:
        plane = jnp.concatenate([edge, plane[: area - cols]], axis=0)
    elif step_y > 0:
        plane = jnp.concatenate([plane[cols:], edge], axis=0)
    return plane


def layer_kernel(
    sizes,
    volume_hbm,
    cotangent_hbm,
    master_hbm,
    moment_hbm,
    second_hbm,
    activation,
    input_grad,
    master_next,
    moment_next,
    second_next,
    volume,
    cotangent,
    master,
    moment,
    second,
    kernel,
    halo,
    grad_halo,
    hidden,
    columns,
    turned,
    local_grad,
    local_sent,
    pair_got,
    chip_sent,
    chip_got,
    own_sum,
    chain_sent,
    chain_got,
    total,
    load_s,
    halo_s,
    halo_r,
    gh_s,
    gh_r,
    ag_s,
    ag_r,
    fw_s,
    fw_r,
    pr_s,
    pr_r,
    ch_s,
    ch_r,
    sl_s,
    sl_r,
    to_s,
    to_r,
    tf_s,
    tf_r,
):
    dps, slabs, planes, area, cols, cells_all = sizes
    chips = slabs // CORES
    width = volume.shape[1]
    rows = master.shape[0]
    half = rows // CORES
    part_rows = half // PARTS
    dp = lax.axis_index("dp")
    slab = lax.axis_index("spatial")
    core = slab % CORES
    chip = slab // CORES
    other = 1 - core
    pair = chip * CORES + other
    block = planes * area

    def copy(src, dst, send, recv, target):
        return pltpu.make_async_remote_copy(
            src_ref=src,
            dst_ref=dst,
            send_sem=send,
            recv_sem=recv,
            device_id=target,
            device_id_type=MESH,
        )

    loads = [
        pltpu.make_async_copy(source, dest, load_s.at[index])
        for index, (source, dest) in enumerate(
            (
                (master_hbm, master),
                (volume_hbm, volume),
                (cotangent_hbm, cotangent),
                (moment_hbm, moment),
                (second_hbm, second),
            )
        )
    ]
    for load in loads:
        load.start()

    barrier = pltpu.get_barrier_semaphore()
    for step in range(1, dps):
        pl.semaphore_signal(
            barrier, inc=1, device_id=((dp + step) % dps, slab), device_id_type=MESH
        )
    for step in range(1, slabs):
        pl.semaphore_signal(
            barrier, inc=1, device_id=(dp, (slab + step) % slabs), device_id_type=MESH
        )

    def kernel_half(shard, which):
        return kernel.at[pl.ds(pl.multiple_of(shard * rows + which * half, TILE), half)]

    loads[0].wait()
    kernel[pl.ds(pl.multiple_of(dp * rows, TILE), rows)] = master[...].astype(jnp.bfloat16)
    pl.semaphore_wait(barrier, dps - 1 + slabs - 1)

    def halo_copy(source, dest, send, recv, side):
        if side == 0:
            return copy(
                source.at[pl.ds(block - area, area)], dest.at[0], send.at[0], recv.at[0], (dp, slab + 1)
            )
        return copy(source.at[pl.ds(0, area)], dest.at[1], send.at[1], recv.at[1], (dp, slab - 1))

    def halo_start(source, dest, send, recv):
        @pl.when(slab < slabs - 1)
        def _():
            halo_copy(source, dest, send, recv, 0).start()

        @pl.when(slab > 0)
        def _():
            halo_copy(source, dest, send, recv, 1).start()

    def halo_sent(source, dest, send, recv):
        @pl.when(slab < slabs - 1)
        def _():
            halo_copy(source, dest, send, recv, 0).wait_send()

        @pl.when(slab > 0)
        def _():
            halo_copy(source, dest, send, recv, 1).wait_send()

    def halo_wait(source, dest, send, recv):
        @pl.when(slab > 0)
        def _():
            halo_copy(source, dest, send, recv, 0).wait_recv()

        @pl.when(slab < slabs - 1)
        def _():
            halo_copy(source, dest, send, recv, 1).wait_recv()

        @pl.when(slab == 0)
        def _():
            dest[0] = jnp.zeros((area, width), jnp.bfloat16)

        @pl.when(slab == slabs - 1)
        def _():
            dest[1] = jnp.zeros((area, width), jnp.bfloat16)

    def gather_copy(shard, target):
        mine = kernel_half(shard, core)
        return copy(mine, mine, ag_s.at[target], ag_r.at[shard], (target, slab))

    def relay_copy(shard, which):
        mine = kernel_half(shard, which)
        return copy(mine, mine, fw_s.at[shard], fw_r.at[shard], (dp, pair))

    for step in range(1, dps):
        gather_copy(dp, (dp + step) % dps).start()
    loads[1].wait()
    halo_start(volume, halo, halo_s, halo_r)

    def put_columns(plane, at, sign, turn):
        plane = plane.astype(jnp.float32)
        for e in range(3):
            for f in range(3):
                moved = shifted(plane, cols, sign * (e - 1), sign * (f - 1)).astype(jnp.bfloat16)
                tap = e * 3 + f
                columns[at * area : (at + 1) * area, tap * width : (tap + 1) * width] = moved
                if turn:
                    turned[tap * width : (tap + 1) * width, at * area : (at + 1) * area] = moved.T

    for plane in range(planes):
        put_columns(volume[plane * area : (plane + 1) * area], plane + 1, 1, True)
    halo_wait(volume, halo, halo_s, halo_r)
    put_columns(halo[0], 0, 1, True)
    put_columns(halo[1], planes + 1, 1, True)

    for step in range(1, dps):
        source = (dp + step) % dps
        gather_copy(source, dp).wait_recv()
        relay_copy(source, core).start()
    for step in range(1, dps):
        relay_copy((dp + step) % dps, other).wait_recv()

    group = 9 * width
    preact = jnp.zeros((block, width), jnp.float32)
    for a in range(3):
        preact = preact + jnp.dot(
            columns[a * area : a * area + block, :],
            kernel[a * group : (a + 1) * group, :],
            preferred_element_type=jnp.float32,
        )
    loads[2].wait()
    sigma = jax.nn.sigmoid(preact)
    activation[...] = (preact * sigma).astype(jnp.bfloat16)
    slope = sigma * (1.0 + preact * (1.0 - sigma))
    hidden[...] = (cotangent[...].astype(jnp.float32) * slope).astype(jnp.bfloat16)

    def rows_of(k):
        return pl.ds(k * part_rows, part_rows)

    def pair_copy(shard, k, which):
        at = pl.ds(pl.multiple_of(shard * rows + which * half + k * part_rows, TILE), part_rows)
        flag = shard * PARTS + k
        return copy(
            local_sent.at[at], pair_got.at[shard, rows_of(k)], pr_s.at[flag], pr_r.at[flag], (dp, pair)
        )

    for a in range(3):
        part = jnp.dot(
            turned[:, a * area : a * area + block],
            hidden[...],
            preferred_element_type=jnp.float32,
        )
        local_grad[a * group : (a + 1) * group, :] = part
        local_sent[a * group : (a + 1) * group, :] = part.astype(jnp.bfloat16)
        if a == 0:
            halo_start(hidden, grad_halo, gh_s, gh_r)

    for k in range(PARTS):
        for step in range(dps):
            pair_copy((dp + step) % dps, k, other).start()

    def chip_rows(shard, k):
        pair_copy(shard, k, core).wait_recv()
        at = pl.multiple_of(shard * rows + core * half + k * part_rows, TILE)
        return local_grad[pl.ds(at, part_rows), :] + pair_got[shard, rows_of(k)].astype(jnp.float32)

    def chip_copy(shard, source, k):
        return copy(
            chip_sent.at[shard, rows_of(k)],
            chip_got.at[source, rows_of(k)],
            ch_s.at[shard * PARTS + k],
            ch_r.at[source * PARTS + k],
            (shard, slab),
        )

    for k in range(PARTS):
        for step in range(1, dps):
            shard = (dp + step) % dps
            chip_sent[shard, rows_of(k)] = chip_rows(shard, k).astype(jnp.bfloat16)
            chip_copy(shard, dp, k).start()
        own_sum[rows_of(k)] = chip_rows(dp, k)

    halo_wait(hidden, grad_halo, gh_s, gh_r)
    for plane in range(planes):
        put_columns(hidden[plane * area : (plane + 1) * area], plane + 1, -1, False)
    put_columns(grad_halo[0], 0, -1, False)
    put_columns(grad_halo[1], planes + 1, -1, False)
    back = jnp.zeros((block, width), jnp.float32)
    for a in range(3):
        for tap in range(9):
            at = (a * 9 + tap) * width
            back = back + lax.dot_general(
                columns[(2 - a) * area : (2 - a) * area + block, tap * width : (tap + 1) * width],
                kernel[at : at + width, :],
                (((1,), (1,)), ((), ())),
                preferred_element_type=jnp.float32,
            )
    input_grad[...] = back.astype(jnp.bfloat16)

    low = chip < chips // 2
    inner = jnp.where(low, chip + 1, chip - 1)
    outer = jnp.where(low, chip - 1, chip + 1)
    is_end = (chip == 0) | (chip == chips - 1)
    is_middle = (chip == chips // 2 - 1) | (chip == chips // 2)
    slot = jnp.where(is_middle, 1, 0)

    def chain_copy(at, k):
        flag = at * PARTS + k
        return copy(
            chain_sent.at[rows_of(k)],
            chain_got.at[at, rows_of(k)],
            sl_s.at[k],
            sl_r.at[flag],
            (dp, inner * CORES + core),
        )

    def total_copy(k):
        ref = total.at[core, rows_of(k)]
        return copy(ref, ref, to_s.at[k], to_r.at[k], (dp, outer * CORES + core))

    def total_relay(k, which):
        ref = total.at[which, rows_of(k)]
        return copy(ref, ref, tf_s.at[k], tf_r.at[k], (dp, pair))

    def reduce_rows(k):
        for step in range(1, dps):
            source = (dp + step) % dps
            chip_copy(dp, source, k).wait_recv()
            own_sum[rows_of(k)] += chip_got[source, rows_of(k)].astype(jnp.float32)

        @pl.when(is_end)
        def _():
            chain_sent[rows_of(k)] = own_sum[rows_of(k)].astype(jnp.bfloat16)
            chain_copy(slot, k).start()

    def pass_inward(k):
        @pl.when(jnp.logical_not(is_end))
        def _():
            chain_copy(0, k).wait_recv()
            chain_sent[rows_of(k)] = (
                own_sum[rows_of(k)] + chain_got[0, rows_of(k)].astype(jnp.float32)
            ).astype(jnp.bfloat16)
            chain_copy(slot, k).start()

    scale = 1.0 / math.sqrt(cells_all)

    def update(k, which):
        at = pl.ds(pl.multiple_of(which * half + k * part_rows, TILE), part_rows)
        grad = total[which, rows_of(k)].astype(jnp.float32) * scale
        old = master[at, :]
        first = 0.9 * moment[at, :] + 0.1 * grad
        square = 0.999 * second[at, :] + 0.001 * grad * grad
        moment_next[at, :] = first
        second_next[at, :] = square
        master_next[at, :] = old - 0.001 * (first / (jnp.sqrt(square) + 1e-08) + 0.01 * old)

    def finish(k):
        @pl.when(is_middle)
        def _():
            chain_copy(1, k).wait_recv()
            total[core, rows_of(k)] = (
                chain_sent[rows_of(k)].astype(jnp.float32)
                + chain_got[1, rows_of(k)].astype(jnp.float32)
            ).astype(jnp.bfloat16)

        @pl.when(jnp.logical_not(is_middle))
        def _():
            total_copy(k).wait_recv()

        @pl.when(jnp.logical_not(is_end))
        def _():
            total_copy(k).start()

        total_relay(k, core).start()
        if k == 0:
            loads[3].wait()
            loads[4].wait()
        update(k, core)

    for k in range(PARTS):
        reduce_rows(k)
        if k >= 1:
            pass_inward(k - 1)
    finish(0)
    pass_inward(PARTS - 1)
    for k in range(PARTS):
        if k >= 1:
            finish(k)
            total_relay(k - 1, other).wait_recv()
            update(k - 1, other)
    total_relay(PARTS - 1, other).wait_recv()
    update(PARTS - 1, other)

    halo_sent(volume, halo, halo_s, halo_r)
    halo_sent(hidden, grad_halo, gh_s, gh_r)
    for step in range(1, dps):
        peer = (dp + step) % dps
        gather_copy(dp, peer).wait_send()
        relay_copy(peer, core).wait_send()
        for k in range(PARTS):
            chip_copy(peer, dp, k).wait_send()
    for k in range(PARTS):
        for shard in range(dps):
            pair_copy(shard, k, other).wait_send()
        chain_copy(slot, k).wait_send()
        total_relay(k, core).wait_send()

        @pl.when(jnp.logical_not(is_end))
        def _():
            total_copy(k).wait_send()


def store_kernel(*refs):
    count = (len(refs) - 1) // 2
    flags = refs[-1]
    stores = [
        pltpu.make_async_copy(refs[index], refs[count + index], flags.at[index])
        for index in range(count)
    ]
    for store in stores:
        store.start()
    for store in stores:
        store.wait()


def per_device(volume, cotangent, master, moment, second):
    _, planes, lines, cols, width = volume.shape
    rows = master.shape[0]
    dps = lax.axis_size("dp")
    slabs = lax.axis_size("spatial")
    chips = slabs // CORES
    area = lines * cols
    block = planes * area
    half = rows // CORES
    cells_all = dps * slabs * block
    bf16, f32 = jnp.bfloat16, jnp.float32
    dma = pltpu.SemaphoreType.DMA
    vmem = pl.BlockSpec(memory_space=pltpu.VMEM)
    sizes = (dps, slabs, planes, area, cols, cells_all)
    out_shape = [
        jax.ShapeDtypeStruct((block, width), bf16),
        jax.ShapeDtypeStruct((block, width), bf16),
        jax.ShapeDtypeStruct((rows, width), f32),
        jax.ShapeDtypeStruct((rows, width), f32),
        jax.ShapeDtypeStruct((rows, width), f32),
    ]
    held = 2 * block * width * 2 + 3 * rows * width * 4
    grant = VMEM_BYTES - held - SLACK
    hbm = pl.BlockSpec(memory_space=pltpu.HBM)
    inside = [pltpu.VMEM(leaf.shape, leaf.dtype) for leaf in out_shape]
    outside = [pltpu.HBM(leaf.shape, leaf.dtype) for leaf in out_shape]
    results = pl.pallas_call(
        functools.partial(layer_kernel, sizes),
        name="layer",
        out_shape=inside,
        in_specs=[hbm] * 5,
        out_specs=[vmem] * 5,
        scratch_shapes=[
            pltpu.VMEM((block, width), bf16),
            pltpu.VMEM((block, width), bf16),
            pltpu.VMEM((rows, width), f32),
            pltpu.VMEM((rows, width), f32),
            pltpu.VMEM((rows, width), f32),
            pltpu.VMEM((dps * rows, width), bf16),
            pltpu.VMEM((2, area, width), bf16),
            pltpu.VMEM((2, area, width), bf16),
            pltpu.VMEM((block, width), bf16),
            pltpu.VMEM((block + 2 * area, 9 * width), bf16),
            pltpu.VMEM((9 * width, block + 2 * area), bf16),
            pltpu.VMEM((dps * rows, width), f32),
            pltpu.VMEM((dps * rows, width), bf16),
            pltpu.VMEM((dps, half, width), bf16),
            pltpu.VMEM((dps, half, width), bf16),
            pltpu.VMEM((dps, half, width), bf16),
            pltpu.VMEM((half, width), f32),
            pltpu.VMEM((half, width), bf16),
            pltpu.VMEM((2, half, width), bf16),
            pltpu.VMEM((CORES, half, width), bf16),
            dma((5,)),
            dma((2,)),
            dma((2,)),
            dma((2,)),
            dma((2,)),
            dma((dps,)),
            dma((dps,)),
            dma((dps,)),
            dma((dps,)),
            dma((dps * PARTS,)),
            dma((dps * PARTS,)),
            dma((dps * PARTS,)),
            dma((dps * PARTS,)),
            dma((PARTS,)),
            dma((2 * PARTS,)),
            dma((PARTS,)),
            dma((PARTS,)),
            dma((PARTS,)),
            dma((PARTS,)),
        ],
        compiler_params=pltpu.CompilerParams(
            collective_id=0, has_side_effects=True, vmem_limit_bytes=32*1024*1024
        ),
    )(
        *(
            pltpu.with_memory_space_constraint(leaf, pltpu.HBM)
            for leaf in (
                volume.reshape(block, width),
                cotangent.reshape(block, width),
                master,
                moment,
                second,
            )
        )
    )
    activation, input_grad, master_next, moment_next, second_next = pl.pallas_call(
        store_kernel,
        name="store",
        out_shape=outside,
        in_specs=[vmem] * 5,
        out_specs=[hbm] * 5,
        scratch_shapes=[dma((5,))],
        compiler_params=pltpu.CompilerParams(vmem_limit_bytes=32*1024*1024),
    )(*results)
    return (
        activation.reshape(volume.shape),
        input_grad.reshape(volume.shape),
        master_next,
        moment_next,
        second_next,
    )


def solution(mesh):
    field = P("dp", "spatial", None, None, None)
    shard = P("dp", None)
    return jax.shard_map(
        per_device,
        mesh=mesh,
        in_specs=(field, field, shard, shard, shard),
        out_specs=(field, field, shard, shard, shard),
        check_vma=False,
    )
```

```python
import functools
import math

import jax
import jax.numpy as jnp
from jax import lax
from jax.experimental import pallas as pl
from jax.experimental.pallas import tpu as pltpu
from jax.sharding import PartitionSpec as P

MESH = pl.DeviceIdType.MESH
TILE = 16
PARTS = 9
LAG = 4
VMEM_BYTES = 67043328
SLACK = 48 * 1024
CORES = 2


def shifted(plane, cols, step_y, step_x):
    area, width = plane.shape
    column = lax.broadcasted_iota(jnp.int32, (area, width), 0) % cols
    if step_x < 0:
        plane = jnp.where(column == 0, 0.0, pltpu.roll(plane, 1, 0))
    elif step_x > 0:
        plane = jnp.where(column == cols - 1, 0.0, pltpu.roll(plane, area - 1, 0))
    edge = jnp.zeros((cols, width), jnp.float32)
    if step_y < 0:
        plane = jnp.concatenate([edge, plane[: area - cols]], axis=0)
    elif step_y > 0:
        plane = jnp.concatenate([plane[cols:], edge], axis=0)
    return plane


def layer_kernel(
    sizes,
    volume_hbm,
    cotangent_hbm,
    master_hbm,
    moment_hbm,
    second_hbm,
    activation,
    input_grad,
    master_next,
    moment_next,
    second_next,
    volume,
    cotangent,
    master,
    moment,
    second,
    kernel,
    halo,
    grad_halo,
    hidden,
    columns,
    turned,
    local_grad,
    local_sent,
    pair_got,
    chip_sent,
    chip_got,
    own_sum,
    chain_sent,
    chain_got,
    total,
    load_s,
    halo_s,
    halo_r,
    gh_s,
    gh_r,
    ag_s,
    ag_r,
    fw_s,
    fw_r,
    pr_s,
    pr_r,
    ch_s,
    ch_r,
    sl_s,
    sl_r,
    to_s,
    to_r,
    tf_s,
    tf_r,
):
    dps, slabs, planes, area, cols, cells_all = sizes
    chips = slabs // CORES
    width = volume.shape[1]
    rows = master.shape[0]
    half = rows // CORES
    part_rows = half // PARTS
    dp = lax.axis_index("dp")
    slab = lax.axis_index("spatial")
    core = slab % CORES
    chip = slab // CORES
    other = 1 - core
    pair = chip * CORES + other
    block = planes * area

    def copy(src, dst, send, recv, target):
        return pltpu.make_async_remote_copy(
            src_ref=src,
            dst_ref=dst,
            send_sem=send,
            recv_sem=recv,
            device_id=target,
            device_id_type=MESH,
        )

    loads = [
        pltpu.make_async_copy(source, dest, load_s.at[index])
        for index, (source, dest) in enumerate(
            (
                (master_hbm, master),
                (volume_hbm, volume),
                (cotangent_hbm, cotangent),
                (moment_hbm, moment),
                (second_hbm, second),
            )
        )
    ]
    for load in loads:
        load.start()

    barrier = pltpu.get_barrier_semaphore()
    for step in range(1, dps):
        pl.semaphore_signal(
            barrier, inc=1, device_id=((dp + step) % dps, slab), device_id_type=MESH
        )
    for gap in (1, 2):

        @pl.when(slab + gap < slabs)
        def _():
            pl.semaphore_signal(barrier, inc=1, device_id=(dp, slab + gap), device_id_type=MESH)

        @pl.when(slab >= gap)
        def _():
            pl.semaphore_signal(barrier, inc=1, device_id=(dp, slab - gap), device_id_type=MESH)

    beside = jnp.minimum(slab, 2) + jnp.minimum(slabs - 1 - slab, 2)
    cut = half // (2 * TILE) * TILE
    spans = ((0, cut), (cut, half - cut))

    def kernel_span(shard, which, p):
        at = pl.multiple_of(shard * rows + which * half + spans[p][0], TILE)
        return kernel.at[pl.ds(at, spans[p][1])]

    loads[0].wait()
    kernel[pl.ds(pl.multiple_of(dp * rows, TILE), rows)] = master[...].astype(jnp.bfloat16)
    pl.semaphore_wait(barrier, dps - 1 + beside)

    def halo_copy(source, dest, send, recv, side):
        if side == 0:
            return copy(
                source.at[pl.ds(block - area, area)], dest.at[0], send.at[0], recv.at[0], (dp, slab + 1)
            )
        return copy(source.at[pl.ds(0, area)], dest.at[1], send.at[1], recv.at[1], (dp, slab - 1))

    def halo_start(source, dest, send, recv):
        @pl.when(slab < slabs - 1)
        def _():
            halo_copy(source, dest, send, recv, 0).start()

        @pl.when(slab > 0)
        def _():
            halo_copy(source, dest, send, recv, 1).start()

    def halo_sent(source, dest, send, recv):
        @pl.when(slab < slabs - 1)
        def _():
            halo_copy(source, dest, send, recv, 0).wait_send()

        @pl.when(slab > 0)
        def _():
            halo_copy(source, dest, send, recv, 1).wait_send()

    def halo_wait(source, dest, send, recv):
        @pl.when(slab > 0)
        def _():
            halo_copy(source, dest, send, recv, 0).wait_recv()

        @pl.when(slab < slabs - 1)
        def _():
            halo_copy(source, dest, send, recv, 1).wait_recv()

        @pl.when(slab == 0)
        def _():
            dest[0] = jnp.zeros((area, width), jnp.bfloat16)

        @pl.when(slab == slabs - 1)
        def _():
            dest[1] = jnp.zeros((area, width), jnp.bfloat16)

    def gather_copy(shard, target, p, lane):
        ref = kernel_span(shard, core, p)
        return copy(ref, ref, ag_s.at[lane * 2 + p], ag_r.at[shard * 2 + p], (target, slab))

    def relay_copy(shard, p, which):
        ref = kernel_span(shard, which, p)
        return copy(ref, ref, fw_s.at[shard * 2 + p], fw_r.at[shard * 2 + p], (dp, pair))

    def relay(shard, p):
        gather_copy(shard, dp, p, shard).wait_recv()
        relay_copy(shard, p, core).start()

    square_grid = dps == 4
    peers = [(dp + step) % dps for step in range(1, dps)]
    sends = [(dp, peer, p, peer) for peer in peers for p in (0, 1)]
    early, late = [], [(peer, p) for peer in peers for p in (0, 1)]
    if square_grid:
        near = dp + 1 - 2 * (dp % 2)
        far = dp + 2 - 4 * (dp // 2)
        across = dps - 1 - dp
        peers = [near, far, across]
        sends = [(dp, near, 0, near), (dp, far, 1, far), (dp, near, 1, near), (dp, far, 0, far)]
        passes = [(near, far, 0, across), (far, near, 1, across)]
        early = [(near, 0), (far, 1)]
        late = [(near, 1), (far, 0), (across, 0), (across, 1)]
    for send in sends:
        gather_copy(*send).start()
    loads[1].wait()
    halo_start(volume, halo, halo_s, halo_r)

    def put_columns(plane, at, sign, turn):
        plane = plane.astype(jnp.float32)
        for e in range(3):
            for f in range(3):
                moved = shifted(plane, cols, sign * (e - 1), sign * (f - 1)).astype(jnp.bfloat16)
                tap = e * 3 + f
                columns[at * area : (at + 1) * area, tap * width : (tap + 1) * width] = moved
                if turn:
                    turned[tap * width : (tap + 1) * width, at * area : (at + 1) * area] = moved.T

    for plane in range(planes):
        put_columns(volume[plane * area : (plane + 1) * area], plane + 1, 1, True)
    for index, (shard, p) in enumerate(early):
        gather_copy(shard, dp, p, shard).wait_recv()
        gather_copy(*passes[index]).start()
        relay_copy(shard, p, core).start()
    halo_wait(volume, halo, halo_s, halo_r)
    put_columns(halo[0], 0, 1, True)
    put_columns(halo[1], planes + 1, 1, True)

    for shard, p in late:
        relay(shard, p)
    for shard, p in early + late:
        relay_copy(shard, p, other).wait_recv()

    group = 9 * width
    preact = jnp.zeros((block, width), jnp.float32)
    for a in range(3):
        preact = preact + jnp.dot(
            columns[a * area : a * area + block, :],
            kernel[a * group : (a + 1) * group, :],
            preferred_element_type=jnp.float32,
        )
    loads[2].wait()
    sigma = jax.nn.sigmoid(preact)
    activation[...] = (preact * sigma).astype(jnp.bfloat16)
    slope = sigma * (1.0 + preact * (1.0 - sigma))
    hidden[...] = (cotangent[...].astype(jnp.float32) * slope).astype(jnp.bfloat16)

    def rows_of(k):
        return pl.ds(k * part_rows, part_rows)

    def pair_copy(shard, k, which):
        at = pl.ds(pl.multiple_of(shard * rows + which * half + k * part_rows, TILE), part_rows)
        flag = shard * PARTS + k
        return copy(
            local_sent.at[at], pair_got.at[shard, rows_of(k)], pr_s.at[flag], pr_r.at[flag], (dp, pair)
        )

    for a in range(3):
        part = jnp.dot(
            turned[:, a * area : a * area + block],
            hidden[...],
            preferred_element_type=jnp.float32,
        )
        local_grad[a * group : (a + 1) * group, :] = part
        local_sent[a * group : (a + 1) * group, :] = part.astype(jnp.bfloat16)
        if a == 0:
            halo_start(hidden, grad_halo, gh_s, gh_r)

    for k in range(PARTS):
        for step in range(dps):
            pair_copy((dp + step) % dps, k, other).start()

    def chip_rows(shard, k):
        pair_copy(shard, k, core).wait_recv()
        at = pl.multiple_of(shard * rows + core * half + k * part_rows, TILE)
        return local_grad[pl.ds(at, part_rows), :] + pair_got[shard, rows_of(k)].astype(jnp.float32)

    def chip_copy(shard, source, k):
        return copy(
            chip_sent.at[shard, rows_of(k)],
            chip_got.at[source, rows_of(k)],
            ch_s.at[shard * PARTS + k],
            ch_r.at[source * PARTS + k],
            (shard, slab),
        )

    for k in range(PARTS):
        for step in range(1, dps):
            shard = (dp + step) % dps
            chip_sent[shard, rows_of(k)] = chip_rows(shard, k).astype(jnp.bfloat16)
            chip_copy(shard, dp, k).start()
        own_sum[rows_of(k)] = chip_rows(dp, k)

    halo_wait(hidden, grad_halo, gh_s, gh_r)
    for plane in range(planes):
        put_columns(hidden[plane * area : (plane + 1) * area], plane + 1, -1, False)
    put_columns(grad_halo[0], 0, -1, False)
    put_columns(grad_halo[1], planes + 1, -1, False)
    back = jnp.zeros((block, width), jnp.float32)
    for a in range(3):
        for tap in range(9):
            at = (a * 9 + tap) * width
            back = back + lax.dot_general(
                columns[(2 - a) * area : (2 - a) * area + block, tap * width : (tap + 1) * width],
                kernel[at : at + width, :],
                (((1,), (1,)), ((), ())),
                preferred_element_type=jnp.float32,
            )
    input_grad[...] = back.astype(jnp.bfloat16)

    low = chip < chips // 2
    inner = jnp.where(low, chip + 1, chip - 1)
    outer = jnp.where(low, chip - 1, chip + 1)
    is_end = (chip == 0) | (chip == chips - 1)
    is_middle = (chip == chips // 2 - 1) | (chip == chips // 2)
    slot = jnp.where(is_middle, 1, 0)

    def chain_copy(at, k):
        flag = at * PARTS + k
        return copy(
            chain_sent.at[rows_of(k)],
            chain_got.at[at, rows_of(k)],
            sl_s.at[k],
            sl_r.at[flag],
            (dp, inner * CORES + core),
        )

    def total_copy(k):
        ref = total.at[core, rows_of(k)]
        return copy(ref, ref, to_s.at[k], to_r.at[k], (dp, outer * CORES + core))

    def total_relay(k, which):
        ref = total.at[which, rows_of(k)]
        return copy(ref, ref, tf_s.at[k], tf_r.at[k], (dp, pair))

    def reduce_rows(k):
        for step in range(1, dps):
            source = (dp + step) % dps
            chip_copy(dp, source, k).wait_recv()
            own_sum[rows_of(k)] += chip_got[source, rows_of(k)].astype(jnp.float32)

        @pl.when(is_end)
        def _():
            chain_sent[rows_of(k)] = own_sum[rows_of(k)].astype(jnp.bfloat16)
            chain_copy(slot, k).start()

    def pass_inward(k):
        @pl.when(jnp.logical_not(is_end))
        def _():
            chain_copy(0, k).wait_recv()
            chain_sent[rows_of(k)] = (
                own_sum[rows_of(k)] + chain_got[0, rows_of(k)].astype(jnp.float32)
            ).astype(jnp.bfloat16)
            chain_copy(slot, k).start()

    scale = 1.0 / math.sqrt(cells_all)

    def update(k, which):
        at = pl.ds(pl.multiple_of(which * half + k * part_rows, TILE), part_rows)
        grad = total[which, rows_of(k)].astype(jnp.float32) * scale
        old = master[at, :]
        first = 0.9 * moment[at, :] + 0.1 * grad
        square = 0.999 * second[at, :] + 0.001 * grad * grad
        moment_next[at, :] = first
        second_next[at, :] = square
        master_next[at, :] = old - 0.001 * (first / (jnp.sqrt(square) + 1e-08) + 0.01 * old)

    def finish(k):
        @pl.when(is_middle)
        def _():
            chain_copy(1, k).wait_recv()
            total[core, rows_of(k)] = (
                chain_sent[rows_of(k)].astype(jnp.float32)
                + chain_got[1, rows_of(k)].astype(jnp.float32)
            ).astype(jnp.bfloat16)

        @pl.when(jnp.logical_not(is_middle))
        def _():
            total_copy(k).wait_recv()

        @pl.when(jnp.logical_not(is_end))
        def _():
            total_copy(k).start()

        total_relay(k, core).start()
        if k == 0:
            loads[3].wait()
            loads[4].wait()
        update(k, core)

    def finish_other(k):
        total_relay(k, other).wait_recv()
        update(k, other)

    for step in range(PARTS + 2 * LAG):
        if step < PARTS:
            reduce_rows(step)
        if 0 <= step - LAG < PARTS:
            pass_inward(step - LAG)
        if 0 <= step - 2 * LAG < PARTS:
            finish(step - 2 * LAG)
        if 0 <= step - 2 * LAG - 2 < PARTS:
            finish_other(step - 2 * LAG - 2)
    for k in range(PARTS - 2, PARTS):
        finish_other(k)

    halo_sent(volume, halo, halo_s, halo_r)
    halo_sent(hidden, grad_halo, gh_s, gh_r)
    for send in sends + (passes if square_grid else []):
        gather_copy(*send).wait_send()
    for shard, p in early + late:
        relay_copy(shard, p, core).wait_send()
    for step in range(1, dps):
        peer = (dp + step) % dps
        for k in range(PARTS):
            chip_copy(peer, dp, k).wait_send()
    for k in range(PARTS):
        for shard in range(dps):
            pair_copy(shard, k, other).wait_send()
        chain_copy(slot, k).wait_send()
        total_relay(k, core).wait_send()

        @pl.when(jnp.logical_not(is_end))
        def _():
            total_copy(k).wait_send()


def store_kernel(*refs):
    count = (len(refs) - 1) // 2
    flags = refs[-1]
    stores = [
        pltpu.make_async_copy(refs[index], refs[count + index], flags.at[index])
        for index in range(count)
    ]
    for store in stores:
        store.start()
    for store in stores:
        store.wait()


def per_device(volume, cotangent, master, moment, second):
    _, planes, lines, cols, width = volume.shape
    rows = master.shape[0]
    dps = lax.axis_size("dp")
    slabs = lax.axis_size("spatial")
    chips = slabs // CORES
    area = lines * cols
    block = planes * area
    half = rows // CORES
    cells_all = dps * slabs * block
    bf16, f32 = jnp.bfloat16, jnp.float32
    dma = pltpu.SemaphoreType.DMA
    vmem = pl.BlockSpec(memory_space=pltpu.VMEM)
    sizes = (dps, slabs, planes, area, cols, cells_all)
    out_shape = [
        jax.ShapeDtypeStruct((block, width), bf16),
        jax.ShapeDtypeStruct((block, width), bf16),
        jax.ShapeDtypeStruct((rows, width), f32),
        jax.ShapeDtypeStruct((rows, width), f32),
        jax.ShapeDtypeStruct((rows, width), f32),
    ]
    held = 2 * block * width * 2 + 3 * rows * width * 4
    grant = VMEM_BYTES - held - SLACK
    hbm = pl.BlockSpec(memory_space=pltpu.HBM)
    inside = [pltpu.VMEM(leaf.shape, leaf.dtype) for leaf in out_shape]
    outside = [pltpu.HBM(leaf.shape, leaf.dtype) for leaf in out_shape]
    results = pl.pallas_call(
        functools.partial(layer_kernel, sizes),
        name="layer",
        out_shape=inside,
        in_specs=[hbm] * 5,
        out_specs=[vmem] * 5,
        scratch_shapes=[
            pltpu.VMEM((block, width), bf16),
            pltpu.VMEM((block, width), bf16),
            pltpu.VMEM((rows, width), f32),
            pltpu.VMEM((rows, width), f32),
            pltpu.VMEM((rows, width), f32),
            pltpu.VMEM((dps * rows, width), bf16),
            pltpu.VMEM((2, area, width), bf16),
            pltpu.VMEM((2, area, width), bf16),
            pltpu.VMEM((block, width), bf16),
            pltpu.VMEM((block + 2 * area, 9 * width), bf16),
            pltpu.VMEM((9 * width, block + 2 * area), bf16),
            pltpu.VMEM((dps * rows, width), f32),
            pltpu.VMEM((dps * rows, width), bf16),
            pltpu.VMEM((dps, half, width), bf16),
            pltpu.VMEM((dps, half, width), bf16),
            pltpu.VMEM((dps, half, width), bf16),
            pltpu.VMEM((half, width), f32),
            pltpu.VMEM((half, width), bf16),
            pltpu.VMEM((2, half, width), bf16),
            pltpu.VMEM((CORES, half, width), bf16),
            dma((5,)),
            dma((2,)),
            dma((2,)),
            dma((2,)),
            dma((2,)),
            dma((2 * dps,)),
            dma((2 * dps,)),
            dma((2 * dps,)),
            dma((2 * dps,)),
            dma((dps * PARTS,)),
            dma((dps * PARTS,)),
            dma((dps * PARTS,)),
            dma((dps * PARTS,)),
            dma((PARTS,)),
            dma((2 * PARTS,)),
            dma((PARTS,)),
            dma((PARTS,)),
            dma((PARTS,)),
            dma((PARTS,)),
        ],
        compiler_params=pltpu.CompilerParams(
            collective_id=0, has_side_effects=True, vmem_limit_bytes=32*1024*1024
        ),
    )(
        *(
            pltpu.with_memory_space_constraint(leaf, pltpu.HBM)
            for leaf in (
                volume.reshape(block, width),
                cotangent.reshape(block, width),
                master,
                moment,
                second,
            )
        )
    )
    activation, input_grad, master_next, moment_next, second_next = pl.pallas_call(
        store_kernel,
        name="store",
        out_shape=outside,
        in_specs=[vmem] * 5,
        out_specs=[hbm] * 5,
        scratch_shapes=[dma((5,))],
        compiler_params=pltpu.CompilerParams(vmem_limit_bytes=32*1024*1024),
    )(*results)
    return (
        activation.reshape(volume.shape),
        input_grad.reshape(volume.shape),
        master_next,
        moment_next,
        second_next,
    )


def solution(mesh):
    field = P("dp", "spatial", None, None, None)
    shard = P("dp", None)
    return jax.shard_map(
        per_device,
        mesh=mesh,
        in_specs=(field, field, shard, shard, shard),
        out_specs=(field, field, shard, shard, shard),
        check_vma=False,
    )
```

```python
import functools
import math

import jax
import jax.numpy as jnp
from jax import lax
from jax.experimental import pallas as pl
from jax.experimental.pallas import tpu as pltpu
from jax.sharding import PartitionSpec as P

MESH = pl.DeviceIdType.MESH
TILE = 16
PARTS = 9
LAG = 4
VMEM_BYTES = 67043328
SLACK = 48 * 1024
CORES = 2


def shifted(plane, cols, step_y, step_x):
    area, width = plane.shape
    column = lax.broadcasted_iota(jnp.int32, (area, width), 0) % cols
    if step_x < 0:
        plane = jnp.where(column == 0, 0.0, pltpu.roll(plane, 1, 0))
    elif step_x > 0:
        plane = jnp.where(column == cols - 1, 0.0, pltpu.roll(plane, area - 1, 0))
    edge = jnp.zeros((cols, width), jnp.float32)
    if step_y < 0:
        plane = jnp.concatenate([edge, plane[: area - cols]], axis=0)
    elif step_y > 0:
        plane = jnp.concatenate([plane[cols:], edge], axis=0)
    return plane


def layer_kernel(
    sizes,
    volume_hbm,
    cotangent_hbm,
    master_hbm,
    moment_hbm,
    second_hbm,
    activation,
    input_grad,
    master_next,
    moment_next,
    second_next,
    volume,
    cotangent,
    master,
    moment,
    second,
    kernel,
    halo,
    grad_halo,
    hidden,
    columns,
    turned,
    local_grad,
    local_sent,
    pair_got,
    chip_sent,
    chip_got,
    own_sum,
    hop_sent,
    hop_got,
    total,
    load_s,
    halo_s,
    halo_r,
    gh_s,
    gh_r,
    ag_s,
    ag_r,
    fw_s,
    fw_r,
    pr_s,
    pr_r,
    ch_s,
    ch_r,
    sl_s,
    sl_r,
    tf_s,
    tf_r,
):
    dps, slabs, planes, area, cols, cells_all = sizes
    chips = slabs // CORES
    width = volume.shape[1]
    rows = master.shape[0]
    half = rows // CORES
    part_rows = half // PARTS
    dp = lax.axis_index("dp")
    slab = lax.axis_index("spatial")
    core = slab % CORES
    chip = slab // CORES
    other = 1 - core
    pair = chip * CORES + other
    block = planes * area

    def copy(src, dst, send, recv, target):
        return pltpu.make_async_remote_copy(
            src_ref=src,
            dst_ref=dst,
            send_sem=send,
            recv_sem=recv,
            device_id=target,
            device_id_type=MESH,
        )

    loads = [
        pltpu.make_async_copy(source, dest, load_s.at[index])
        for index, (source, dest) in enumerate(
            (
                (master_hbm, master),
                (volume_hbm, volume),
                (cotangent_hbm, cotangent),
                (moment_hbm, moment),
                (second_hbm, second),
            )
        )
    ]
    for load in loads:
        load.start()

    barrier = pltpu.get_barrier_semaphore()
    for step in range(1, dps):
        pl.semaphore_signal(
            barrier, inc=1, device_id=((dp + step) % dps, slab), device_id_type=MESH
        )
    @pl.when(slab + 1 < slabs)
    def _():
        pl.semaphore_signal(barrier, inc=1, device_id=(dp, slab + 1), device_id_type=MESH)

    @pl.when(slab >= 1)
    def _():
        pl.semaphore_signal(barrier, inc=1, device_id=(dp, slab - 1), device_id_type=MESH)

    hops = chips.bit_length() - 1
    partners = [(chip + gap * (1 - 2 * (chip // gap % 2))) * CORES + core for gap in [2**h for h in range(hops)]]
    for partner in partners:
        pl.semaphore_signal(barrier, inc=1, device_id=(dp, partner), device_id_type=MESH)
    beside = jnp.minimum(slab, 1) + jnp.minimum(slabs - 1 - slab, 1) + hops
    cut = half // (2 * TILE) * TILE
    spans = ((0, cut), (cut, half - cut))

    def kernel_span(shard, which, p):
        at = pl.multiple_of(shard * rows + which * half + spans[p][0], TILE)
        return kernel.at[pl.ds(at, spans[p][1])]

    loads[0].wait()
    kernel[pl.ds(pl.multiple_of(dp * rows, TILE), rows)] = master[...].astype(jnp.bfloat16)
    pl.semaphore_wait(barrier, dps - 1 + beside)

    def halo_copy(source, dest, send, recv, side):
        if side == 0:
            return copy(
                source.at[pl.ds(block - area, area)], dest.at[0], send.at[0], recv.at[0], (dp, slab + 1)
            )
        return copy(source.at[pl.ds(0, area)], dest.at[1], send.at[1], recv.at[1], (dp, slab - 1))

    def halo_start(source, dest, send, recv):
        @pl.when(slab < slabs - 1)
        def _():
            halo_copy(source, dest, send, recv, 0).start()

        @pl.when(slab > 0)
        def _():
            halo_copy(source, dest, send, recv, 1).start()

    def halo_sent(source, dest, send, recv):
        @pl.when(slab < slabs - 1)
        def _():
            halo_copy(source, dest, send, recv, 0).wait_send()

        @pl.when(slab > 0)
        def _():
            halo_copy(source, dest, send, recv, 1).wait_send()

    def halo_wait(source, dest, send, recv):
        @pl.when(slab > 0)
        def _():
            halo_copy(source, dest, send, recv, 0).wait_recv()

        @pl.when(slab < slabs - 1)
        def _():
            halo_copy(source, dest, send, recv, 1).wait_recv()

        @pl.when(slab == 0)
        def _():
            dest[0] = jnp.zeros((area, width), jnp.bfloat16)

        @pl.when(slab == slabs - 1)
        def _():
            dest[1] = jnp.zeros((area, width), jnp.bfloat16)

    def gather_copy(shard, target, p, lane):
        ref = kernel_span(shard, core, p)
        return copy(ref, ref, ag_s.at[lane * 2 + p], ag_r.at[shard * 2 + p], (target, slab))

    def relay_copy(shard, p, which):
        ref = kernel_span(shard, which, p)
        return copy(ref, ref, fw_s.at[shard * 2 + p], fw_r.at[shard * 2 + p], (dp, pair))

    def relay(shard, p):
        gather_copy(shard, dp, p, shard).wait_recv()
        relay_copy(shard, p, core).start()

    square_grid = dps == 4
    peers = [(dp + step) % dps for step in range(1, dps)]
    sends = [(dp, peer, p, peer) for peer in peers for p in (0, 1)]
    early, late = [], [(peer, p) for peer in peers for p in (0, 1)]
    if square_grid:
        near = dp + 1 - 2 * (dp % 2)
        far = dp + 2 - 4 * (dp // 2)
        across = dps - 1 - dp
        peers = [near, far, across]
        sends = [(dp, near, 0, near), (dp, far, 1, far), (dp, near, 1, near), (dp, far, 0, far)]
        passes = [(near, far, 0, across), (far, near, 1, across)]
        early = [(near, 0), (far, 1)]
        late = [(near, 1), (far, 0), (across, 0), (across, 1)]
    for send in sends:
        gather_copy(*send).start()
    loads[1].wait()
    halo_start(volume, halo, halo_s, halo_r)

    def put_columns(plane, at, sign, turn):
        plane = plane.astype(jnp.float32)
        for e in range(3):
            for f in range(3):
                moved = shifted(plane, cols, sign * (e - 1), sign * (f - 1)).astype(jnp.bfloat16)
                tap = e * 3 + f
                columns[at * area : (at + 1) * area, tap * width : (tap + 1) * width] = moved
                if turn:
                    turned[tap * width : (tap + 1) * width, at * area : (at + 1) * area] = moved.T

    for plane in range(planes):
        put_columns(volume[plane * area : (plane + 1) * area], plane + 1, 1, True)
    for index, (shard, p) in enumerate(early):
        gather_copy(shard, dp, p, shard).wait_recv()
        gather_copy(*passes[index]).start()
        relay_copy(shard, p, core).start()
    halo_wait(volume, halo, halo_s, halo_r)
    put_columns(halo[0], 0, 1, True)
    put_columns(halo[1], planes + 1, 1, True)

    for shard, p in late:
        relay(shard, p)
    for shard, p in early + late:
        relay_copy(shard, p, other).wait_recv()

    group = 9 * width
    preact = jnp.zeros((block, width), jnp.float32)
    for a in range(3):
        preact = preact + jnp.dot(
            columns[a * area : a * area + block, :],
            kernel[a * group : (a + 1) * group, :],
            preferred_element_type=jnp.float32,
        )
    loads[2].wait()
    sigma = jax.nn.sigmoid(preact)
    activation[...] = (preact * sigma).astype(jnp.bfloat16)
    slope = sigma * (1.0 + preact * (1.0 - sigma))
    hidden[...] = (cotangent[...].astype(jnp.float32) * slope).astype(jnp.bfloat16)

    def rows_of(k):
        return pl.ds(k * part_rows, part_rows)

    def pair_copy(shard, k, which):
        at = pl.ds(pl.multiple_of(shard * rows + which * half + k * part_rows, TILE), part_rows)
        flag = shard * PARTS + k
        return copy(
            local_sent.at[at], pair_got.at[shard, rows_of(k)], pr_s.at[flag], pr_r.at[flag], (dp, pair)
        )

    for a in range(3):
        part = jnp.dot(
            turned[:, a * area : a * area + block],
            hidden[...],
            preferred_element_type=jnp.float32,
        )
        local_grad[a * group : (a + 1) * group, :] = part
        local_sent[a * group : (a + 1) * group, :] = part.astype(jnp.bfloat16)
        if a == 0:
            halo_start(hidden, grad_halo, gh_s, gh_r)

    for k in range(PARTS):
        for step in range(dps):
            pair_copy((dp + step) % dps, k, other).start()

    def chip_rows(shard, k):
        pair_copy(shard, k, core).wait_recv()
        at = pl.multiple_of(shard * rows + core * half + k * part_rows, TILE)
        return local_grad[pl.ds(at, part_rows), :] + pair_got[shard, rows_of(k)].astype(jnp.float32)

    def chip_copy(shard, source, k):
        return copy(
            chip_sent.at[shard, rows_of(k)],
            chip_got.at[source, rows_of(k)],
            ch_s.at[shard * PARTS + k],
            ch_r.at[source * PARTS + k],
            (shard, slab),
        )

    for k in range(PARTS):
        for step in range(1, dps):
            shard = (dp + step) % dps
            chip_sent[shard, rows_of(k)] = chip_rows(shard, k).astype(jnp.bfloat16)
            chip_copy(shard, dp, k).start()
        own_sum[rows_of(k)] = chip_rows(dp, k)

    halo_wait(hidden, grad_halo, gh_s, gh_r)
    for plane in range(planes):
        put_columns(hidden[plane * area : (plane + 1) * area], plane + 1, -1, False)
    put_columns(grad_halo[0], 0, -1, False)
    put_columns(grad_halo[1], planes + 1, -1, False)
    back = jnp.zeros((block, width), jnp.float32)
    for a in range(3):
        for tap in range(9):
            at = (a * 9 + tap) * width
            back = back + lax.dot_general(
                columns[(2 - a) * area : (2 - a) * area + block, tap * width : (tap + 1) * width],
                kernel[at : at + width, :],
                (((1,), (1,)), ((), ())),
                preferred_element_type=jnp.float32,
            )
    input_grad[...] = back.astype(jnp.bfloat16)

    def hop_copy(h, k):
        flag = h * PARTS + k
        return copy(
            hop_sent.at[h, rows_of(k)],
            hop_got.at[h, rows_of(k)],
            sl_s.at[flag],
            sl_r.at[flag],
            (dp, partners[h]),
        )

    def total_relay(k, which):
        ref = total.at[which, rows_of(k)]
        return copy(ref, ref, tf_s.at[k], tf_r.at[k], (dp, pair))

    def reduce_rows(k):
        for step in range(1, dps):
            source = (dp + step) % dps
            chip_copy(dp, source, k).wait_recv()
            own_sum[rows_of(k)] += chip_got[source, rows_of(k)].astype(jnp.float32)

        hop_sent[0, rows_of(k)] = own_sum[rows_of(k)].astype(jnp.bfloat16)
        hop_copy(0, k).start()

    def hop_sum(h, k):
        hop_copy(h, k).wait_recv()
        mine = hop_sent[h, rows_of(k)].astype(jnp.float32)
        return (mine + hop_got[h, rows_of(k)].astype(jnp.float32)).astype(jnp.bfloat16)

    def pass_on(h, k):
        hop_sent[h, rows_of(k)] = hop_sum(h - 1, k)
        hop_copy(h, k).start()

    scale = 1.0 / math.sqrt(cells_all)

    def update(k, which):
        at = pl.ds(pl.multiple_of(which * half + k * part_rows, TILE), part_rows)
        grad = total[which, rows_of(k)].astype(jnp.float32) * scale
        old = master[at, :]
        first = 0.9 * moment[at, :] + 0.1 * grad
        square = 0.999 * second[at, :] + 0.001 * grad * grad
        moment_next[at, :] = first
        second_next[at, :] = square
        master_next[at, :] = old - 0.001 * (first / (jnp.sqrt(square) + 1e-08) + 0.01 * old)

    def finish(k):
        total[core, rows_of(k)] = hop_sum(hops - 1, k)
        total_relay(k, core).start()
        if k == 0:
            loads[3].wait()
            loads[4].wait()
        update(k, core)

    def finish_other(k):
        total_relay(k, other).wait_recv()
        update(k, other)

    last = hops * LAG
    for step in range(PARTS + last):
        if step < PARTS:
            reduce_rows(step)
        for h in range(1, hops):
            if 0 <= step - h * LAG < PARTS:
                pass_on(h, step - h * LAG)
        if 0 <= step - last < PARTS:
            finish(step - last)
        if 0 <= step - last - 2 < PARTS:
            finish_other(step - last - 2)
    for k in range(PARTS - 2, PARTS):
        finish_other(k)

    halo_sent(volume, halo, halo_s, halo_r)
    halo_sent(hidden, grad_halo, gh_s, gh_r)
    for send in sends + (passes if square_grid else []):
        gather_copy(*send).wait_send()
    for shard, p in early + late:
        relay_copy(shard, p, core).wait_send()
    for step in range(1, dps):
        peer = (dp + step) % dps
        for k in range(PARTS):
            chip_copy(peer, dp, k).wait_send()
    for k in range(PARTS):
        for shard in range(dps):
            pair_copy(shard, k, other).wait_send()
        for h in range(hops):
            hop_copy(h, k).wait_send()
        total_relay(k, core).wait_send()


def store_kernel(*refs):
    count = (len(refs) - 1) // 2
    flags = refs[-1]
    stores = [
        pltpu.make_async_copy(refs[index], refs[count + index], flags.at[index])
        for index in range(count)
    ]
    for store in stores:
        store.start()
    for store in stores:
        store.wait()


def per_device(volume, cotangent, master, moment, second):
    _, planes, lines, cols, width = volume.shape
    rows = master.shape[0]
    dps = lax.axis_size("dp")
    slabs = lax.axis_size("spatial")
    chips = slabs // CORES
    hops = chips.bit_length() - 1
    area = lines * cols
    block = planes * area
    half = rows // CORES
    cells_all = dps * slabs * block
    bf16, f32 = jnp.bfloat16, jnp.float32
    dma = pltpu.SemaphoreType.DMA
    vmem = pl.BlockSpec(memory_space=pltpu.VMEM)
    sizes = (dps, slabs, planes, area, cols, cells_all)
    out_shape = [
        jax.ShapeDtypeStruct((block, width), bf16),
        jax.ShapeDtypeStruct((block, width), bf16),
        jax.ShapeDtypeStruct((rows, width), f32),
        jax.ShapeDtypeStruct((rows, width), f32),
        jax.ShapeDtypeStruct((rows, width), f32),
    ]
    held = 2 * block * width * 2 + 3 * rows * width * 4
    grant = VMEM_BYTES - held - SLACK
    hbm = pl.BlockSpec(memory_space=pltpu.HBM)
    inside = [pltpu.VMEM(leaf.shape, leaf.dtype) for leaf in out_shape]
    outside = [pltpu.HBM(leaf.shape, leaf.dtype) for leaf in out_shape]
    results = pl.pallas_call(
        functools.partial(layer_kernel, sizes),
        name="layer",
        out_shape=inside,
        in_specs=[hbm] * 5,
        out_specs=[vmem] * 5,
        scratch_shapes=[
            pltpu.VMEM((block, width), bf16),
            pltpu.VMEM((block, width), bf16),
            pltpu.VMEM((rows, width), f32),
            pltpu.VMEM((rows, width), f32),
            pltpu.VMEM((rows, width), f32),
            pltpu.VMEM((dps * rows, width), bf16),
            pltpu.VMEM((2, area, width), bf16),
            pltpu.VMEM((2, area, width), bf16),
            pltpu.VMEM((block, width), bf16),
            pltpu.VMEM((block + 2 * area, 9 * width), bf16),
            pltpu.VMEM((9 * width, block + 2 * area), bf16),
            pltpu.VMEM((dps * rows, width), f32),
            pltpu.VMEM((dps * rows, width), bf16),
            pltpu.VMEM((dps, half, width), bf16),
            pltpu.VMEM((dps, half, width), bf16),
            pltpu.VMEM((dps, half, width), bf16),
            pltpu.VMEM((half, width), f32),
            pltpu.VMEM((hops, half, width), bf16),
            pltpu.VMEM((hops, half, width), bf16),
            pltpu.VMEM((CORES, half, width), bf16),
            dma((5,)),
            dma((2,)),
            dma((2,)),
            dma((2,)),
            dma((2,)),
            dma((2 * dps,)),
            dma((2 * dps,)),
            dma((2 * dps,)),
            dma((2 * dps,)),
            dma((dps * PARTS,)),
            dma((dps * PARTS,)),
            dma((dps * PARTS,)),
            dma((dps * PARTS,)),
            dma((hops * PARTS,)),
            dma((hops * PARTS,)),
            dma((PARTS,)),
            dma((PARTS,)),
        ],
        compiler_params=pltpu.CompilerParams(
            collective_id=0, has_side_effects=True, vmem_limit_bytes=32*1024*1024
        ),
    )(
        *(
            pltpu.with_memory_space_constraint(leaf, pltpu.HBM)
            for leaf in (
                volume.reshape(block, width),
                cotangent.reshape(block, width),
                master,
                moment,
                second,
            )
        )
    )
    activation, input_grad, master_next, moment_next, second_next = pl.pallas_call(
        store_kernel,
        name="store",
        out_shape=outside,
        in_specs=[vmem] * 5,
        out_specs=[hbm] * 5,
        scratch_shapes=[dma((5,))],
        compiler_params=pltpu.CompilerParams(vmem_limit_bytes=32*1024*1024),
    )(*results)
    return (
        activation.reshape(volume.shape),
        input_grad.reshape(volume.shape),
        master_next,
        moment_next,
        second_next,
    )


def solution(mesh):
    field = P("dp", "spatial", None, None, None)
    shard = P("dp", None)
    return jax.shard_map(
        per_device,
        mesh=mesh,
        in_specs=(field, field, shard, shard, shard),
        out_specs=(field, field, shard, shard, shard),
        check_vma=False,
    )
```

```python
import functools
import math

import jax
import jax.numpy as jnp
from jax import lax
from jax.experimental import pallas as pl
from jax.experimental.pallas import tpu as pltpu
from jax.sharding import PartitionSpec as P

MESH = pl.DeviceIdType.MESH
TILE = 16
PARTS = 3
LAG = 2
VMEM_BYTES = 67043328
SLACK = 48 * 1024
CORES = 2


def shifted(plane, cols, step_y, step_x):
    area, width = plane.shape
    column = lax.broadcasted_iota(jnp.int32, (area, width), 0) % cols
    if step_x < 0:
        plane = jnp.where(column == 0, 0.0, pltpu.roll(plane, 1, 0))
    elif step_x > 0:
        plane = jnp.where(column == cols - 1, 0.0, pltpu.roll(plane, area - 1, 0))
    edge = jnp.zeros((cols, width), jnp.float32)
    if step_y < 0:
        plane = jnp.concatenate([edge, plane[: area - cols]], axis=0)
    elif step_y > 0:
        plane = jnp.concatenate([plane[cols:], edge], axis=0)
    return plane


def layer_kernel(
    sizes,
    volume_hbm,
    cotangent_hbm,
    master_hbm,
    moment_hbm,
    second_hbm,
    activation,
    input_grad,
    master_next,
    moment_next,
    second_next,
    volume,
    cotangent,
    master,
    moment,
    second,
    kernel,
    halo,
    grad_halo,
    hidden,
    columns,
    turned,
    local_grad,
    local_sent,
    pair_got,
    chip_sent,
    chip_got,
    own_sum,
    hop_sent,
    hop_got,
    total,
    load_s,
    halo_s,
    halo_r,
    gh_s,
    gh_r,
    ag_s,
    ag_r,
    fw_s,
    fw_r,
    pr_s,
    pr_r,
    ch_s,
    ch_r,
    sl_s,
    sl_r,
    tf_s,
    tf_r,
):
    dps, slabs, planes, area, cols, cells_all = sizes
    chips = slabs // CORES
    width = volume.shape[1]
    rows = master.shape[0]
    half = rows // CORES
    part_rows = half // PARTS
    dp = lax.axis_index("dp")
    slab = lax.axis_index("spatial")
    core = slab % CORES
    chip = slab // CORES
    other = 1 - core
    pair = chip * CORES + other
    block = planes * area

    def copy(src, dst, send, recv, target):
        return pltpu.make_async_remote_copy(
            src_ref=src,
            dst_ref=dst,
            send_sem=send,
            recv_sem=recv,
            device_id=target,
            device_id_type=MESH,
        )

    loads = [
        pltpu.make_async_copy(source, dest, load_s.at[index])
        for index, (source, dest) in enumerate(
            (
                (master_hbm, master),
                (volume_hbm, volume),
                (cotangent_hbm, cotangent),
                (moment_hbm, moment),
                (second_hbm, second),
            )
        )
    ]
    for load in loads:
        load.start()

    barrier = pltpu.get_barrier_semaphore()
    for step in range(1, dps):
        pl.semaphore_signal(
            barrier, inc=1, device_id=((dp + step) % dps, slab), device_id_type=MESH
        )
    @pl.when(slab + 1 < slabs)
    def _():
        pl.semaphore_signal(barrier, inc=1, device_id=(dp, slab + 1), device_id_type=MESH)

    @pl.when(slab >= 1)
    def _():
        pl.semaphore_signal(barrier, inc=1, device_id=(dp, slab - 1), device_id_type=MESH)

    hops = chips.bit_length() - 1
    partners = [(chip + gap * (1 - 2 * (chip // gap % 2))) * CORES + core for gap in [2**h for h in range(hops)]]
    for partner in partners:
        pl.semaphore_signal(barrier, inc=1, device_id=(dp, partner), device_id_type=MESH)
    beside = jnp.minimum(slab, 1) + jnp.minimum(slabs - 1 - slab, 1) + hops
    cut = half // (2 * TILE) * TILE
    spans = ((0, cut), (cut, half - cut))

    def kernel_span(shard, which, p):
        at = pl.multiple_of(shard * rows + which * half + spans[p][0], TILE)
        return kernel.at[pl.ds(at, spans[p][1])]

    loads[0].wait()
    kernel[pl.ds(pl.multiple_of(dp * rows, TILE), rows)] = master[...].astype(jnp.bfloat16)
    pl.semaphore_wait(barrier, dps - 1 + beside)

    def halo_copy(source, dest, send, recv, side):
        if side == 0:
            return copy(
                source.at[pl.ds(block - area, area)], dest.at[0], send.at[0], recv.at[0], (dp, slab + 1)
            )
        return copy(source.at[pl.ds(0, area)], dest.at[1], send.at[1], recv.at[1], (dp, slab - 1))

    def halo_start(source, dest, send, recv):
        @pl.when(slab < slabs - 1)
        def _():
            halo_copy(source, dest, send, recv, 0).start()

        @pl.when(slab > 0)
        def _():
            halo_copy(source, dest, send, recv, 1).start()

    def halo_sent(source, dest, send, recv):
        @pl.when(slab < slabs - 1)
        def _():
            halo_copy(source, dest, send, recv, 0).wait_send()

        @pl.when(slab > 0)
        def _():
            halo_copy(source, dest, send, recv, 1).wait_send()

    def halo_wait(source, dest, send, recv):
        @pl.when(slab > 0)
        def _():
            halo_copy(source, dest, send, recv, 0).wait_recv()

        @pl.when(slab < slabs - 1)
        def _():
            halo_copy(source, dest, send, recv, 1).wait_recv()

        @pl.when(slab == 0)
        def _():
            dest[0] = jnp.zeros((area, width), jnp.bfloat16)

        @pl.when(slab == slabs - 1)
        def _():
            dest[1] = jnp.zeros((area, width), jnp.bfloat16)

    def gather_copy(shard, target, p, lane):
        ref = kernel_span(shard, core, p)
        return copy(ref, ref, ag_s.at[lane * 2 + p], ag_r.at[shard * 2 + p], (target, slab))

    def relay_copy(shard, p, which):
        ref = kernel_span(shard, which, p)
        return copy(ref, ref, fw_s.at[shard * 2 + p], fw_r.at[shard * 2 + p], (dp, pair))

    def relay(shard, p):
        gather_copy(shard, dp, p, shard).wait_recv()
        relay_copy(shard, p, core).start()

    square_grid = dps == 4
    peers = [(dp + step) % dps for step in range(1, dps)]
    sends = [(dp, peer, p, peer) for peer in peers for p in (0, 1)]
    early, late = [], [(peer, p) for peer in peers for p in (0, 1)]
    if square_grid:
        near = dp + 1 - 2 * (dp % 2)
        far = dp + 2 - 4 * (dp // 2)
        across = dps - 1 - dp
        peers = [near, far, across]
        sends = [(dp, near, 0, near), (dp, far, 1, far), (dp, near, 1, near), (dp, far, 0, far)]
        passes = [(near, far, 0, across), (far, near, 1, across)]
        early = [(near, 0), (far, 1)]
        late = [(near, 1), (far, 0), (across, 0), (across, 1)]
    for send in sends:
        gather_copy(*send).start()
    loads[1].wait()
    halo_start(volume, halo, halo_s, halo_r)

    def put_columns(plane, at, sign, turn):
        plane = plane.astype(jnp.float32)
        for e in range(3):
            for f in range(3):
                moved = shifted(plane, cols, sign * (e - 1), sign * (f - 1)).astype(jnp.bfloat16)
                tap = e * 3 + f
                columns[at * area : (at + 1) * area, tap * width : (tap + 1) * width] = moved
                if turn:
                    turned[tap * width : (tap + 1) * width, at * area : (at + 1) * area] = moved.T

    for plane in range(planes):
        put_columns(volume[plane * area : (plane + 1) * area], plane + 1, 1, True)
    for index, (shard, p) in enumerate(early):
        gather_copy(shard, dp, p, shard).wait_recv()
        gather_copy(*passes[index]).start()
        relay_copy(shard, p, core).start()
    halo_wait(volume, halo, halo_s, halo_r)
    put_columns(halo[0], 0, 1, True)
    put_columns(halo[1], planes + 1, 1, True)

    for shard, p in late:
        relay(shard, p)
    for shard, p in early + late:
        relay_copy(shard, p, other).wait_recv()

    group = 9 * width
    preact = jnp.zeros((block, width), jnp.float32)
    for a in range(3):
        preact = preact + jnp.dot(
            columns[a * area : a * area + block, :],
            kernel[a * group : (a + 1) * group, :],
            preferred_element_type=jnp.float32,
        )
    loads[2].wait()
    sigma = jax.nn.sigmoid(preact)
    activation[...] = (preact * sigma).astype(jnp.bfloat16)
    slope = sigma * (1.0 + preact * (1.0 - sigma))
    hidden[...] = (cotangent[...].astype(jnp.float32) * slope).astype(jnp.bfloat16)

    def rows_of(k):
        return pl.ds(k * part_rows, part_rows)

    def pair_copy(shard, k, which):
        at = pl.ds(pl.multiple_of(shard * rows + which * half + k * part_rows, TILE), part_rows)
        flag = shard * PARTS + k
        return copy(
            local_sent.at[at], pair_got.at[shard, rows_of(k)], pr_s.at[flag], pr_r.at[flag], (dp, pair)
        )

    for a in range(3):
        part = jnp.dot(
            turned[:, a * area : a * area + block],
            hidden[...],
            preferred_element_type=jnp.float32,
        )
        local_grad[a * group : (a + 1) * group, :] = part
        local_sent[a * group : (a + 1) * group, :] = part.astype(jnp.bfloat16)
        if a == 0:
            halo_start(hidden, grad_halo, gh_s, gh_r)

    for k in range(PARTS):
        for step in range(dps):
            pair_copy((dp + step) % dps, k, other).start()

    def chip_rows(shard, k):
        pair_copy(shard, k, core).wait_recv()
        at = pl.multiple_of(shard * rows + core * half + k * part_rows, TILE)
        return local_grad[pl.ds(at, part_rows), :] + pair_got[shard, rows_of(k)].astype(jnp.float32)

    def chip_copy(shard, source, k):
        return copy(
            chip_sent.at[shard, rows_of(k)],
            chip_got.at[source, rows_of(k)],
            ch_s.at[shard * PARTS + k],
            ch_r.at[source * PARTS + k],
            (shard, slab),
        )

    for k in range(PARTS):
        for step in range(1, dps):
            shard = (dp + step) % dps
            chip_sent[shard, rows_of(k)] = chip_rows(shard, k).astype(jnp.bfloat16)
            chip_copy(shard, dp, k).start()
        own_sum[rows_of(k)] = chip_rows(dp, k)

    halo_wait(hidden, grad_halo, gh_s, gh_r)
    for plane in range(planes):
        put_columns(hidden[plane * area : (plane + 1) * area], plane + 1, -1, False)
    put_columns(grad_halo[0], 0, -1, False)
    put_columns(grad_halo[1], planes + 1, -1, False)
    back = jnp.zeros((block, width), jnp.float32)
    for a in range(3):
        for tap in range(9):
            at = (a * 9 + tap) * width
            back = back + lax.dot_general(
                columns[(2 - a) * area : (2 - a) * area + block, tap * width : (tap + 1) * width],
                kernel[at : at + width, :],
                (((1,), (1,)), ((), ())),
                preferred_element_type=jnp.float32,
            )
    input_grad[...] = back.astype(jnp.bfloat16)

    def hop_copy(h, k):
        flag = h * PARTS + k
        return copy(
            hop_sent.at[h, rows_of(k)],
            hop_got.at[h, rows_of(k)],
            sl_s.at[flag],
            sl_r.at[flag],
            (dp, partners[h]),
        )

    def total_relay(k, which):
        ref = total.at[which, rows_of(k)]
        return copy(ref, ref, tf_s.at[k], tf_r.at[k], (dp, pair))

    def reduce_rows(k):
        for step in range(1, dps):
            source = (dp + step) % dps
            chip_copy(dp, source, k).wait_recv()
            own_sum[rows_of(k)] += chip_got[source, rows_of(k)].astype(jnp.float32)

        hop_sent[0, rows_of(k)] = own_sum[rows_of(k)].astype(jnp.bfloat16)
        hop_copy(0, k).start()

    def hop_sum(h, k):
        hop_copy(h, k).wait_recv()
        mine = hop_sent[h, rows_of(k)].astype(jnp.float32)
        return (mine + hop_got[h, rows_of(k)].astype(jnp.float32)).astype(jnp.bfloat16)

    def pass_on(h, k):
        hop_sent[h, rows_of(k)] = hop_sum(h - 1, k)
        hop_copy(h, k).start()

    scale = 1.0 / math.sqrt(cells_all)

    def update(k, which):
        at = pl.ds(pl.multiple_of(which * half + k * part_rows, TILE), part_rows)
        grad = total[which, rows_of(k)].astype(jnp.float32) * scale
        old = master[at, :]
        first = 0.9 * moment[at, :] + 0.1 * grad
        square = 0.999 * second[at, :] + 0.001 * grad * grad
        moment_next[at, :] = first
        second_next[at, :] = square
        master_next[at, :] = old - 0.001 * (first / (jnp.sqrt(square) + 1e-08) + 0.01 * old)

    def finish(k):
        total[core, rows_of(k)] = hop_sum(hops - 1, k)
        total_relay(k, core).start()
        if k == 0:
            loads[3].wait()
            loads[4].wait()
        update(k, core)

    def finish_other(k):
        total_relay(k, other).wait_recv()
        update(k, other)

    last = hops * LAG
    for step in range(PARTS + last):
        if step < PARTS:
            reduce_rows(step)
        for h in range(1, hops):
            if 0 <= step - h * LAG < PARTS:
                pass_on(h, step - h * LAG)
        if 0 <= step - last < PARTS:
            finish(step - last)
        if 0 <= step - last - 2 < PARTS:
            finish_other(step - last - 2)
    for k in range(PARTS - 2, PARTS):
        finish_other(k)

    halo_sent(volume, halo, halo_s, halo_r)
    halo_sent(hidden, grad_halo, gh_s, gh_r)
    for send in sends + (passes if square_grid else []):
        gather_copy(*send).wait_send()
    for shard, p in early + late:
        relay_copy(shard, p, core).wait_send()
    for step in range(1, dps):
        peer = (dp + step) % dps
        for k in range(PARTS):
            chip_copy(peer, dp, k).wait_send()
    for k in range(PARTS):
        for shard in range(dps):
            pair_copy(shard, k, other).wait_send()
        for h in range(hops):
            hop_copy(h, k).wait_send()
        total_relay(k, core).wait_send()


def store_kernel(*refs):
    count = (len(refs) - 1) // 2
    flags = refs[-1]
    stores = [
        pltpu.make_async_copy(refs[index], refs[count + index], flags.at[index])
        for index in range(count)
    ]
    for store in stores:
        store.start()
    for store in stores:
        store.wait()


def per_device(volume, cotangent, master, moment, second):
    _, planes, lines, cols, width = volume.shape
    rows = master.shape[0]
    dps = lax.axis_size("dp")
    slabs = lax.axis_size("spatial")
    chips = slabs // CORES
    hops = chips.bit_length() - 1
    area = lines * cols
    block = planes * area
    half = rows // CORES
    cells_all = dps * slabs * block
    bf16, f32 = jnp.bfloat16, jnp.float32
    dma = pltpu.SemaphoreType.DMA
    vmem = pl.BlockSpec(memory_space=pltpu.VMEM)
    sizes = (dps, slabs, planes, area, cols, cells_all)
    out_shape = [
        jax.ShapeDtypeStruct((block, width), bf16),
        jax.ShapeDtypeStruct((block, width), bf16),
        jax.ShapeDtypeStruct((rows, width), f32),
        jax.ShapeDtypeStruct((rows, width), f32),
        jax.ShapeDtypeStruct((rows, width), f32),
    ]
    held = 2 * block * width * 2 + 3 * rows * width * 4
    grant = VMEM_BYTES - held - SLACK
    hbm = pl.BlockSpec(memory_space=pltpu.HBM)
    inside = [pltpu.VMEM(leaf.shape, leaf.dtype) for leaf in out_shape]
    outside = [pltpu.HBM(leaf.shape, leaf.dtype) for leaf in out_shape]
    results = pl.pallas_call(
        functools.partial(layer_kernel, sizes),
        name="layer",
        out_shape=inside,
        in_specs=[hbm] * 5,
        out_specs=[vmem] * 5,
        scratch_shapes=[
            pltpu.VMEM((block, width), bf16),
            pltpu.VMEM((block, width), bf16),
            pltpu.VMEM((rows, width), f32),
            pltpu.VMEM((rows, width), f32),
            pltpu.VMEM((rows, width), f32),
            pltpu.VMEM((dps * rows, width), bf16),
            pltpu.VMEM((2, area, width), bf16),
            pltpu.VMEM((2, area, width), bf16),
            pltpu.VMEM((block, width), bf16),
            pltpu.VMEM((block + 2 * area, 9 * width), bf16),
            pltpu.VMEM((9 * width, block + 2 * area), bf16),
            pltpu.VMEM((dps * rows, width), f32),
            pltpu.VMEM((dps * rows, width), bf16),
            pltpu.VMEM((dps, half, width), bf16),
            pltpu.VMEM((dps, half, width), bf16),
            pltpu.VMEM((dps, half, width), bf16),
            pltpu.VMEM((half, width), f32),
            pltpu.VMEM((hops, half, width), bf16),
            pltpu.VMEM((hops, half, width), bf16),
            pltpu.VMEM((CORES, half, width), bf16),
            dma((5,)),
            dma((2,)),
            dma((2,)),
            dma((2,)),
            dma((2,)),
            dma((2 * dps,)),
            dma((2 * dps,)),
            dma((2 * dps,)),
            dma((2 * dps,)),
            dma((dps * PARTS,)),
            dma((dps * PARTS,)),
            dma((dps * PARTS,)),
            dma((dps * PARTS,)),
            dma((hops * PARTS,)),
            dma((hops * PARTS,)),
            dma((PARTS,)),
            dma((PARTS,)),
        ],
        compiler_params=pltpu.CompilerParams(
            collective_id=0, has_side_effects=True, vmem_limit_bytes=32*1024*1024
        ),
    )(
        *(
            pltpu.with_memory_space_constraint(leaf, pltpu.HBM)
            for leaf in (
                volume.reshape(block, width),
                cotangent.reshape(block, width),
                master,
                moment,
                second,
            )
        )
    )
    activation, input_grad, master_next, moment_next, second_next = pl.pallas_call(
        store_kernel,
        name="store",
        out_shape=outside,
        in_specs=[vmem] * 5,
        out_specs=[hbm] * 5,
        scratch_shapes=[dma((5,))],
        compiler_params=pltpu.CompilerParams(vmem_limit_bytes=32*1024*1024),
    )(*results)
    return (
        activation.reshape(volume.shape),
        input_grad.reshape(volume.shape),
        master_next,
        moment_next,
        second_next,
    )


def solution(mesh):
    field = P("dp", "spatial", None, None, None)
    shard = P("dp", None)
    return jax.shard_map(
        per_device,
        mesh=mesh,
        in_specs=(field, field, shard, shard, shard),
        out_specs=(field, field, shard, shard, shard),
        check_vma=False,
    )
```

```python
import functools
import math

import jax
import jax.numpy as jnp
from jax import lax
from jax.experimental import pallas as pl
from jax.experimental.pallas import tpu as pltpu
from jax.sharding import PartitionSpec as P

MESH = pl.DeviceIdType.MESH
TILE = 16
PARTS = 3
LAG = 3
VMEM_BYTES = 67043328
SLACK = 48 * 1024
CORES = 2


def shifted(plane, cols, step_y, step_x):
    area, width = plane.shape
    column = lax.broadcasted_iota(jnp.int32, (area, width), 0) % cols
    if step_x < 0:
        plane = jnp.where(column == 0, 0.0, pltpu.roll(plane, 1, 0))
    elif step_x > 0:
        plane = jnp.where(column == cols - 1, 0.0, pltpu.roll(plane, area - 1, 0))
    edge = jnp.zeros((cols, width), jnp.float32)
    if step_y < 0:
        plane = jnp.concatenate([edge, plane[: area - cols]], axis=0)
    elif step_y > 0:
        plane = jnp.concatenate([plane[cols:], edge], axis=0)
    return plane


def layer_kernel(
    sizes,
    volume_hbm,
    cotangent_hbm,
    master_hbm,
    moment_hbm,
    second_hbm,
    activation,
    input_grad,
    master_next,
    moment_next,
    second_next,
    volume,
    cotangent,
    master,
    moment,
    second,
    kernel,
    halo,
    grad_halo,
    hidden,
    columns,
    turned,
    local_grad,
    local_sent,
    pair_got,
    chip_sent,
    chip_got,
    own_sum,
    hop_sent,
    hop_got,
    total,
    load_s,
    halo_s,
    halo_r,
    gh_s,
    gh_r,
    ag_s,
    ag_r,
    fw_s,
    fw_r,
    pr_s,
    pr_r,
    ch_s,
    ch_r,
    sl_s,
    sl_r,
    tf_s,
    tf_r,
):
    dps, slabs, planes, area, cols, cells_all = sizes
    chips = slabs // CORES
    width = volume.shape[1]
    rows = master.shape[0]
    half = rows // CORES
    part_rows = half // PARTS
    dp = lax.axis_index("dp")
    slab = lax.axis_index("spatial")
    core = slab % CORES
    chip = slab // CORES
    other = 1 - core
    pair = chip * CORES + other
    block = planes * area

    def copy(src, dst, send, recv, target):
        return pltpu.make_async_remote_copy(
            src_ref=src,
            dst_ref=dst,
            send_sem=send,
            recv_sem=recv,
            device_id=target,
            device_id_type=MESH,
        )

    loads = [
        pltpu.make_async_copy(source, dest, load_s.at[index])
        for index, (source, dest) in enumerate(
            (
                (master_hbm, master),
                (volume_hbm, volume),
                (cotangent_hbm, cotangent),
                (moment_hbm, moment),
                (second_hbm, second),
            )
        )
    ]
    for load in loads:
        load.start()

    barrier = pltpu.get_barrier_semaphore()
    for step in range(1, dps):
        pl.semaphore_signal(
            barrier, inc=1, device_id=((dp + step) % dps, slab), device_id_type=MESH
        )
    @pl.when(slab + 1 < slabs)
    def _():
        pl.semaphore_signal(barrier, inc=1, device_id=(dp, slab + 1), device_id_type=MESH)

    @pl.when(slab >= 1)
    def _():
        pl.semaphore_signal(barrier, inc=1, device_id=(dp, slab - 1), device_id_type=MESH)

    hops = chips.bit_length() - 1
    partners = [(chip + gap * (1 - 2 * (chip // gap % 2))) * CORES + core for gap in [2**h for h in range(hops)]]
    for partner in partners:
        pl.semaphore_signal(barrier, inc=1, device_id=(dp, partner), device_id_type=MESH)
    beside = jnp.minimum(slab, 1) + jnp.minimum(slabs - 1 - slab, 1) + hops
    cut = half // (2 * TILE) * TILE
    spans = ((0, cut), (cut, half - cut))

    def kernel_span(shard, which, p):
        at = pl.multiple_of(shard * rows + which * half + spans[p][0], TILE)
        return kernel.at[pl.ds(at, spans[p][1])]

    loads[0].wait()
    kernel[pl.ds(pl.multiple_of(dp * rows, TILE), rows)] = master[...].astype(jnp.bfloat16)
    pl.semaphore_wait(barrier, dps - 1 + beside)

    def halo_copy(source, dest, send, recv, side):
        if side == 0:
            return copy(
                source.at[pl.ds(block - area, area)], dest.at[0], send.at[0], recv.at[0], (dp, slab + 1)
            )
        return copy(source.at[pl.ds(0, area)], dest.at[1], send.at[1], recv.at[1], (dp, slab - 1))

    def halo_start(source, dest, send, recv):
        @pl.when(slab < slabs - 1)
        def _():
            halo_copy(source, dest, send, recv, 0).start()

        @pl.when(slab > 0)
        def _():
            halo_copy(source, dest, send, recv, 1).start()

    def halo_sent(source, dest, send, recv):
        @pl.when(slab < slabs - 1)
        def _():
            halo_copy(source, dest, send, recv, 0).wait_send()

        @pl.when(slab > 0)
        def _():
            halo_copy(source, dest, send, recv, 1).wait_send()

    def halo_wait(source, dest, send, recv):
        @pl.when(slab > 0)
        def _():
            halo_copy(source, dest, send, recv, 0).wait_recv()

        @pl.when(slab < slabs - 1)
        def _():
            halo_copy(source, dest, send, recv, 1).wait_recv()

        @pl.when(slab == 0)
        def _():
            dest[0] = jnp.zeros((area, width), jnp.bfloat16)

        @pl.when(slab == slabs - 1)
        def _():
            dest[1] = jnp.zeros((area, width), jnp.bfloat16)

    def gather_copy(shard, target, p, lane):
        ref = kernel_span(shard, core, p)
        return copy(ref, ref, ag_s.at[lane * 2 + p], ag_r.at[shard * 2 + p], (target, slab))

    def relay_copy(shard, p, which):
        ref = kernel_span(shard, which, p)
        return copy(ref, ref, fw_s.at[shard * 2 + p], fw_r.at[shard * 2 + p], (dp, pair))

    def relay(shard, p):
        gather_copy(shard, dp, p, shard).wait_recv()
        relay_copy(shard, p, core).start()

    square_grid = dps == 4
    peers = [(dp + step) % dps for step in range(1, dps)]
    sends = [(dp, peer, p, peer) for peer in peers for p in (0, 1)]
    early, late = [], [(peer, p) for peer in peers for p in (0, 1)]
    if square_grid:
        near = dp + 1 - 2 * (dp % 2)
        far = dp + 2 - 4 * (dp // 2)
        across = dps - 1 - dp
        peers = [near, far, across]
        sends = [(dp, near, 0, near), (dp, far, 1, far), (dp, near, 1, near), (dp, far, 0, far)]
        passes = [(near, far, 0, across), (far, near, 1, across)]
        early = [(near, 0), (far, 1)]
        late = [(near, 1), (far, 0), (across, 0), (across, 1)]
    for send in sends:
        gather_copy(*send).start()
    loads[1].wait()
    halo_start(volume, halo, halo_s, halo_r)

    def put_columns(plane, at, sign, turn):
        plane = plane.astype(jnp.float32)
        for e in range(3):
            for f in range(3):
                moved = shifted(plane, cols, sign * (e - 1), sign * (f - 1)).astype(jnp.bfloat16)
                tap = e * 3 + f
                columns[at * area : (at + 1) * area, tap * width : (tap + 1) * width] = moved
                if turn:
                    turned[tap * width : (tap + 1) * width, at * area : (at + 1) * area] = moved.T

    for plane in range(planes):
        put_columns(volume[plane * area : (plane + 1) * area], plane + 1, 1, True)
    for index, (shard, p) in enumerate(early):
        gather_copy(shard, dp, p, shard).wait_recv()
        gather_copy(*passes[index]).start()
        relay_copy(shard, p, core).start()
    halo_wait(volume, halo, halo_s, halo_r)
    put_columns(halo[0], 0, 1, True)
    put_columns(halo[1], planes + 1, 1, True)

    for shard, p in late:
        relay(shard, p)
    for shard, p in early + late:
        relay_copy(shard, p, other).wait_recv()

    group = 9 * width
    preact = jnp.zeros((block, width), jnp.float32)
    for a in range(3):
        preact = preact + jnp.dot(
            columns[a * area : a * area + block, :],
            kernel[a * group : (a + 1) * group, :],
            preferred_element_type=jnp.float32,
        )
    loads[2].wait()
    sigma = jax.nn.sigmoid(preact)
    activation[...] = (preact * sigma).astype(jnp.bfloat16)
    slope = sigma * (1.0 + preact * (1.0 - sigma))
    hidden[...] = (cotangent[...].astype(jnp.float32) * slope).astype(jnp.bfloat16)

    def rows_of(k):
        return pl.ds(k * part_rows, part_rows)

    def pair_copy(shard, k, which):
        at = pl.ds(pl.multiple_of(shard * rows + which * half + k * part_rows, TILE), part_rows)
        flag = shard * PARTS + k
        return copy(
            local_sent.at[at], pair_got.at[shard, rows_of(k)], pr_s.at[flag], pr_r.at[flag], (dp, pair)
        )

    for a in range(3):
        part = jnp.dot(
            turned[:, a * area : a * area + block],
            hidden[...],
            preferred_element_type=jnp.float32,
        )
        local_grad[a * group : (a + 1) * group, :] = part
        local_sent[a * group : (a + 1) * group, :] = part.astype(jnp.bfloat16)
        if a == 0:
            halo_start(hidden, grad_halo, gh_s, gh_r)

    for k in range(PARTS):
        for step in range(dps):
            pair_copy((dp + step) % dps, k, other).start()

    def chip_rows(shard, k):
        pair_copy(shard, k, core).wait_recv()
        at = pl.multiple_of(shard * rows + core * half + k * part_rows, TILE)
        return local_grad[pl.ds(at, part_rows), :] + pair_got[shard, rows_of(k)].astype(jnp.float32)

    def chip_copy(shard, source, k):
        return copy(
            chip_sent.at[shard, rows_of(k)],
            chip_got.at[source, rows_of(k)],
            ch_s.at[shard * PARTS + k],
            ch_r.at[source * PARTS + k],
            (shard, slab),
        )

    for k in range(PARTS):
        for step in range(1, dps):
            shard = (dp + step) % dps
            chip_sent[shard, rows_of(k)] = chip_rows(shard, k).astype(jnp.bfloat16)
            chip_copy(shard, dp, k).start()
        own_sum[rows_of(k)] = chip_rows(dp, k)

    halo_wait(hidden, grad_halo, gh_s, gh_r)
    for plane in range(planes):
        put_columns(hidden[plane * area : (plane + 1) * area], plane + 1, -1, False)
    put_columns(grad_halo[0], 0, -1, False)
    put_columns(grad_halo[1], planes + 1, -1, False)
    back = jnp.zeros((block, width), jnp.float32)
    for a in range(3):
        for tap in range(9):
            at = (a * 9 + tap) * width
            back = back + lax.dot_general(
                columns[(2 - a) * area : (2 - a) * area + block, tap * width : (tap + 1) * width],
                kernel[at : at + width, :],
                (((1,), (1,)), ((), ())),
                preferred_element_type=jnp.float32,
            )
    input_grad[...] = back.astype(jnp.bfloat16)

    def hop_copy(h, k):
        flag = h * PARTS + k
        return copy(
            hop_sent.at[h, rows_of(k)],
            hop_got.at[h, rows_of(k)],
            sl_s.at[flag],
            sl_r.at[flag],
            (dp, partners[h]),
        )

    def total_relay(k, which):
        ref = total.at[which, rows_of(k)]
        return copy(ref, ref, tf_s.at[k], tf_r.at[k], (dp, pair))

    def reduce_rows(k):
        for step in range(1, dps):
            source = (dp + step) % dps
            chip_copy(dp, source, k).wait_recv()
            own_sum[rows_of(k)] += chip_got[source, rows_of(k)].astype(jnp.float32)

        hop_sent[0, rows_of(k)] = own_sum[rows_of(k)].astype(jnp.bfloat16)
        hop_copy(0, k).start()

    def hop_sum(h, k):
        hop_copy(h, k).wait_recv()
        mine = hop_sent[h, rows_of(k)].astype(jnp.float32)
        return (mine + hop_got[h, rows_of(k)].astype(jnp.float32)).astype(jnp.bfloat16)

    def pass_on(h, k):
        hop_sent[h, rows_of(k)] = hop_sum(h - 1, k)
        hop_copy(h, k).start()

    scale = 1.0 / math.sqrt(cells_all)

    def update(k, which):
        at = pl.ds(pl.multiple_of(which * half + k * part_rows, TILE), part_rows)
        grad = total[which, rows_of(k)].astype(jnp.float32) * scale
        old = master[at, :]
        first = 0.9 * moment[at, :] + 0.1 * grad
        square = 0.999 * second[at, :] + 0.001 * grad * grad
        moment_next[at, :] = first
        second_next[at, :] = square
        master_next[at, :] = old - 0.001 * (first / (jnp.sqrt(square) + 1e-08) + 0.01 * old)

    def finish(k):
        total[core, rows_of(k)] = hop_sum(hops - 1, k)
        total_relay(k, core).start()
        if k == 0:
            loads[3].wait()
            loads[4].wait()
        update(k, core)

    def finish_other(k):
        total_relay(k, other).wait_recv()
        update(k, other)

    last = hops * LAG
    for step in range(PARTS + last):
        if step < PARTS:
            reduce_rows(step)
        for h in range(1, hops):
            if 0 <= step - h * LAG < PARTS:
                pass_on(h, step - h * LAG)
        if 0 <= step - last < PARTS:
            finish(step - last)
        if 0 <= step - last - 2 < PARTS:
            finish_other(step - last - 2)
    for k in range(PARTS - 2, PARTS):
        finish_other(k)

    halo_sent(volume, halo, halo_s, halo_r)
    halo_sent(hidden, grad_halo, gh_s, gh_r)
    for send in sends + (passes if square_grid else []):
        gather_copy(*send).wait_send()
    for shard, p in early + late:
        relay_copy(shard, p, core).wait_send()
    for step in range(1, dps):
        peer = (dp + step) % dps
        for k in range(PARTS):
            chip_copy(peer, dp, k).wait_send()
    for k in range(PARTS):
        for shard in range(dps):
            pair_copy(shard, k, other).wait_send()
        for h in range(hops):
            hop_copy(h, k).wait_send()
        total_relay(k, core).wait_send()


def store_kernel(*refs):
    count = (len(refs) - 1) // 2
    flags = refs[-1]
    stores = [
        pltpu.make_async_copy(refs[index], refs[count + index], flags.at[index])
        for index in range(count)
    ]
    for store in stores:
        store.start()
    for store in stores:
        store.wait()


def per_device(volume, cotangent, master, moment, second):
    _, planes, lines, cols, width = volume.shape
    rows = master.shape[0]
    dps = lax.axis_size("dp")
    slabs = lax.axis_size("spatial")
    chips = slabs // CORES
    hops = chips.bit_length() - 1
    area = lines * cols
    block = planes * area
    half = rows // CORES
    cells_all = dps * slabs * block
    bf16, f32 = jnp.bfloat16, jnp.float32
    dma = pltpu.SemaphoreType.DMA
    vmem = pl.BlockSpec(memory_space=pltpu.VMEM)
    sizes = (dps, slabs, planes, area, cols, cells_all)
    out_shape = [
        jax.ShapeDtypeStruct((block, width), bf16),
        jax.ShapeDtypeStruct((block, width), bf16),
        jax.ShapeDtypeStruct((rows, width), f32),
        jax.ShapeDtypeStruct((rows, width), f32),
        jax.ShapeDtypeStruct((rows, width), f32),
    ]
    held = 2 * block * width * 2 + 3 * rows * width * 4
    grant = VMEM_BYTES - held - SLACK
    hbm = pl.BlockSpec(memory_space=pltpu.HBM)
    inside = [pltpu.VMEM(leaf.shape, leaf.dtype) for leaf in out_shape]
    outside = [pltpu.HBM(leaf.shape, leaf.dtype) for leaf in out_shape]
    results = pl.pallas_call(
        functools.partial(layer_kernel, sizes),
        name="layer",
        out_shape=inside,
        in_specs=[hbm] * 5,
        out_specs=[vmem] * 5,
        scratch_shapes=[
            pltpu.VMEM((block, width), bf16),
            pltpu.VMEM((block, width), bf16),
            pltpu.VMEM((rows, width), f32),
            pltpu.VMEM((rows, width), f32),
            pltpu.VMEM((rows, width), f32),
            pltpu.VMEM((dps * rows, width), bf16),
            pltpu.VMEM((2, area, width), bf16),
            pltpu.VMEM((2, area, width), bf16),
            pltpu.VMEM((block, width), bf16),
            pltpu.VMEM((block + 2 * area, 9 * width), bf16),
            pltpu.VMEM((9 * width, block + 2 * area), bf16),
            pltpu.VMEM((dps * rows, width), f32),
            pltpu.VMEM((dps * rows, width), bf16),
            pltpu.VMEM((dps, half, width), bf16),
            pltpu.VMEM((dps, half, width), bf16),
            pltpu.VMEM((dps, half, width), bf16),
            pltpu.VMEM((half, width), f32),
            pltpu.VMEM((hops, half, width), bf16),
            pltpu.VMEM((hops, half, width), bf16),
            pltpu.VMEM((CORES, half, width), bf16),
            dma((5,)),
            dma((2,)),
            dma((2,)),
            dma((2,)),
            dma((2,)),
            dma((2 * dps,)),
            dma((2 * dps,)),
            dma((2 * dps,)),
            dma((2 * dps,)),
            dma((dps * PARTS,)),
            dma((dps * PARTS,)),
            dma((dps * PARTS,)),
            dma((dps * PARTS,)),
            dma((hops * PARTS,)),
            dma((hops * PARTS,)),
            dma((PARTS,)),
            dma((PARTS,)),
        ],
        compiler_params=pltpu.CompilerParams(
            collective_id=0, has_side_effects=True, vmem_limit_bytes=32*1024*1024
        ),
    )(
        *(
            pltpu.with_memory_space_constraint(leaf, pltpu.HBM)
            for leaf in (
                volume.reshape(block, width),
                cotangent.reshape(block, width),
                master,
                moment,
                second,
            )
        )
    )
    activation, input_grad, master_next, moment_next, second_next = pl.pallas_call(
        store_kernel,
        name="store",
        out_shape=outside,
        in_specs=[vmem] * 5,
        out_specs=[hbm] * 5,
        scratch_shapes=[dma((5,))],
        compiler_params=pltpu.CompilerParams(vmem_limit_bytes=32*1024*1024),
    )(*results)
    return (
        activation.reshape(volume.shape),
        input_grad.reshape(volume.shape),
        master_next,
        moment_next,
        second_next,
    )


def solution(mesh):
    field = P("dp", "spatial", None, None, None)
    shard = P("dp", None)
    return jax.shard_map(
        per_device,
        mesh=mesh,
        in_specs=(field, field, shard, shard, shard),
        out_specs=(field, field, shard, shard, shard),
        check_vma=False,
    )
```
